32 devices in a mesh: dp: 2 (over x), tp: 4 (over z), sp: 4 (over y, core).
Axes of the slice: x: 2, y: 2, z: 4, core: 2. Of those that a mesh axis runs over, the one named last changes fastest.
Arguments:
- step_emb: bfloat16 [4, 32, 2048], P(None, 'dp'), parts along dimension 1
- v_cache: bfloat16 [2, 32, 1024, 2048], P(None, 'dp', 'sp', 'tp'), parts along dimension 1
- z_cache: bfloat16 [2, 32, 1024, 2048], P(None, 'dp', 'sp', 'tp'), parts along dimension 1
- short_state: bfloat16 [2, 32, 2, 3, 2048], P(None, 'dp', None, None, 'tp'), parts along dimension 1
- w_in: bfloat16 [2, 2048, 3, 2048], P(None, None, None, 'tp')
- b_in: float32 [2, 3, 2048], P(None, None, 'tp')
- short_taps: float32 [2, 3, 3, 2048], P(None, None, None, 'tp')
- long_filt: float32 [2, 2, 1024, 2048], P(None, None, None, 'tp')
- skip_gain: float32 [2, 2, 2048], P(None, None, 'tp')
- w_out: bfloat16 [2, 2048, 2048], P(None, 'tp')
- b_out: float32 [2, 2048], replicated
- w_up: bfloat16 [2, 2048, 8192], P(None, None, 'tp')
- w_down: bfloat16 [2, 8192, 2048], P(None, 'tp')
Outputs:
- output 1: float32 [4, 32, 2048], P(None, 'dp'), parts along dimension 1
- output 2: bfloat16 [2, 32, 1024, 2048], P(None, 'dp', 'sp', 'tp'), parts along dimension 1
- output 3: bfloat16 [2, 32, 1024, 2048], P(None, 'dp', 'sp', 'tp'), parts along dimension 1
- output 4: bfloat16 [2, 32, 2, 3, 2048], P(None, 'dp', None, None, 'tp'), parts along dimension 1
There are 2 independent parts. The reference program is written for one: setup_inputs(seed, part) draws one part's arguments, and reference() takes and returns one part's arrays. A program takes and returns all parts, laid end to end along the dimension named above; an argument that names none is the same for every part.
All inputs are finite; a program needn't handle non-finite values.
Results may differ from the reference program's by a relative error of at most 0.0113581.
Values sent between devices are 32-bit elements.
A program may use at most 1 GiB of HBM per device.

```python
import jax
import jax.numpy as jnp
from jax import lax

MODEL_DIM = 2048
MLP_DIM = 8192
NUM_SEQ = 16
CACHE_LEN = 1024
NUM_STEPS = 4
NUM_LAYERS = 2
START_POS = CACHE_LEN * 3 // 4


def setup_inputs(seed: int = 0, part: int = 0) -> dict:
    root_key = jax.random.key(seed)
    part_root, shared_root = jax.random.split(root_key)
    part_keys = jax.random.split(jax.random.fold_in(part_root, part), 4)
    shared_keys = jax.random.split(shared_root, 9)
    filled_mask = (jnp.arange(CACHE_LEN) < START_POS)[None, None, :, None]
    lag_pos = jnp.arange(CACHE_LEN).astype(jnp.float32)
    decay_rows = jnp.exp(-0.5 * lag_pos / CACHE_LEN)[:, None]
    cache_shape = (NUM_LAYERS, NUM_SEQ, CACHE_LEN, MODEL_DIM)
    step_emb = jax.random.normal(part_keys[0], (NUM_STEPS, NUM_SEQ, MODEL_DIM), jnp.float32)
    v_cache = jax.random.normal(part_keys[1], cache_shape, jnp.float32) * filled_mask
    z_cache = jax.random.normal(part_keys[2], cache_shape, jnp.float32) * filled_mask
    short_state = jax.random.normal(part_keys[3], (NUM_LAYERS, NUM_SEQ, 2, 3, MODEL_DIM), jnp.float32)
    w_in = jax.random.normal(shared_keys[0], (NUM_LAYERS, MODEL_DIM, 3, MODEL_DIM), jnp.float32) * MODEL_DIM ** -0.5
    b_in = 0.5 * jax.random.normal(shared_keys[1], (NUM_LAYERS, 3, MODEL_DIM), jnp.float32)
    short_taps = 0.6 * jax.random.normal(shared_keys[2], (NUM_LAYERS, 3, 3, MODEL_DIM), jnp.float32)
    long_filt = jax.random.normal(shared_keys[3], (NUM_LAYERS, 2, CACHE_LEN, MODEL_DIM), jnp.float32) * decay_rows * (1.4 * CACHE_LEN ** -0.5)
    skip_gain = 0.6 * jax.random.normal(shared_keys[4], (NUM_LAYERS, 2, MODEL_DIM), jnp.float32)
    w_out = jax.random.normal(shared_keys[5], (NUM_LAYERS, MODEL_DIM, MODEL_DIM), jnp.float32) * MODEL_DIM ** -0.5
    b_out = 0.5 * jax.random.normal(shared_keys[6], (NUM_LAYERS, MODEL_DIM), jnp.float32)
    w_up = jax.random.normal(shared_keys[7], (NUM_LAYERS, MODEL_DIM, MLP_DIM), jnp.float32) * MODEL_DIM ** -0.5
    w_down = jax.random.normal(shared_keys[8], (NUM_LAYERS, MLP_DIM, MODEL_DIM), jnp.float32) * (1.5 * MLP_DIM ** -0.5)
    return {
        "step_emb": step_emb.astype(jnp.bfloat16),
        "v_cache": v_cache.astype(jnp.bfloat16),
        "z_cache": z_cache.astype(jnp.bfloat16),
        "short_state": short_state.astype(jnp.bfloat16),
        "w_in": w_in.astype(jnp.bfloat16),
        "b_in": b_in,
        "short_taps": short_taps,
        "long_filt": long_filt,
        "skip_gain": skip_gain,
        "w_out": w_out.astype(jnp.bfloat16),
        "b_out": b_out,
        "w_up": w_up.astype(jnp.bfloat16),
        "w_down": w_down.astype(jnp.bfloat16),
    }


def layer_norm(rows_in):
    mean_val = jnp.mean(rows_in, axis=-1, keepdims=True)
    centered = rows_in - mean_val
    var_val = jnp.mean(centered * centered, axis=-1, keepdims=True)
    return centered * lax.rsqrt(var_val + 1e-5)


def long_conv(cache_rows, filt_rows, pos_now):
    lag_pos = pos_now - jnp.arange(CACHE_LEN)
    taps_now = jnp.take(filt_rows, jnp.maximum(lag_pos, 0), axis=0)
    taps_now = jnp.where((lag_pos >= 0)[:, None], taps_now, 0.0)
    return jnp.sum(cache_rows.astype(jnp.float32) * taps_now[None], axis=1)


def reference(step_emb, v_cache, z_cache, short_state, w_in, b_in, short_taps, long_filt, skip_gain, w_out, b_out, w_up, w_down):
    def one_step(carry, step_in):
        v_list, z_list, state_list = carry
        emb_row, step_idx = step_in
        pos_now = START_POS + step_idx
        hidden = emb_row.astype(jnp.float32)
        new_v = []
        new_z = []
        new_state = []
        for layer_idx in range(NUM_LAYERS):
            normed = layer_norm(hidden).astype(jnp.bfloat16)
            w_flat = w_in[layer_idx].reshape(MODEL_DIM, 3 * MODEL_DIM)
            proj_row = jnp.dot(normed, w_flat, preferred_element_type=jnp.float32).reshape(-1, 3, MODEL_DIM)
            proj_row = (proj_row + b_in[layer_idx]).astype(jnp.bfloat16)
            prev_state = state_list[layer_idx]
            tap_rows = short_taps[layer_idx]
            mixed_rows = (tap_rows[0] * proj_row.astype(jnp.float32)
                          + tap_rows[1] * prev_state[:, 1].astype(jnp.float32)
                          + tap_rows[2] * prev_state[:, 0].astype(jnp.float32))
            new_state.append(jnp.stack([prev_state[:, 1], proj_row], axis=1))
            value_row = mixed_rows[:, 2].astype(jnp.bfloat16)
            v_layer = lax.dynamic_update_slice(v_list[layer_idx], value_row[:, None, :], (0, pos_now, 0))
            long_one = long_conv(v_layer, long_filt[layer_idx, 0], pos_now) + skip_gain[layer_idx, 0] * value_row.astype(jnp.float32)
            z_row = (mixed_rows[:, 0] * long_one).astype(jnp.bfloat16)
            z_layer = lax.dynamic_update_slice(z_list[layer_idx], z_row[:, None, :], (0, pos_now, 0))
            long_two = long_conv(z_layer, long_filt[layer_idx, 1], pos_now) + skip_gain[layer_idx, 1] * z_row.astype(jnp.float32)
            y_row = (mixed_rows[:, 1] * long_two).astype(jnp.bfloat16)
            hidden = hidden + jnp.dot(y_row, w_out[layer_idx], preferred_element_type=jnp.float32) + b_out[layer_idx]
            inner_act = jax.nn.gelu(jnp.dot(layer_norm(hidden).astype(jnp.bfloat16), w_up[layer_idx], preferred_element_type=jnp.float32)).astype(jnp.bfloat16)
            hidden = hidden + jnp.dot(inner_act, w_down[layer_idx], preferred_element_type=jnp.float32)
            new_v.append(v_layer)
            new_z.append(z_layer)
        return (tuple(new_v), tuple(new_z), tuple(new_state)), hidden

    init_carry = (
        tuple(v_cache[layer_idx] for layer_idx in range(NUM_LAYERS)),
        tuple(z_cache[layer_idx] for layer_idx in range(NUM_LAYERS)),
        tuple(short_state[layer_idx] for layer_idx in range(NUM_LAYERS)),
    )
    final_carry, hiddens = lax.scan(one_step, init_carry, (step_emb, jnp.arange(NUM_STEPS)))
    v_out, z_out, state_out = final_carry
    return (hiddens, jnp.stack(v_out), jnp.stack(z_out), jnp.stack(state_out))
```

```python
import jax
import jax.numpy as jnp
from jax import lax
from jax.sharding import PartitionSpec as P

NUM_STEPS = 4
NUM_LAYERS = 2


def layer_norm(rows_in):
    mean_val = jnp.mean(rows_in, axis=-1, keepdims=True)
    centered = rows_in - mean_val
    var_val = jnp.mean(centered * centered, axis=-1, keepdims=True)
    return centered * lax.rsqrt(var_val + 1e-5)


def gather_rows(rows, axis, zero):
    return lax.all_gather(rows.astype(jnp.float32), "sp", axis=axis, tiled=True) + zero


def solution(mesh):
    sp_size = mesh.shape["sp"]

    def device_fn(step_emb, v_cache, z_cache, short_state, w_in, b_in, short_taps, long_filt, skip_gain, w_out, b_out, w_up, w_down):
        f32 = jnp.float32
        num_seq = v_cache.shape[1]
        shard_len = v_cache.shape[2]
        start_pos = shard_len * sp_size * 3 // 4
        sp_idx = lax.axis_index("sp")
        shard_start = sp_idx * shard_len
        own = num_seq // sp_size
        lag_pos = start_pos + NUM_STEPS - 1 - shard_start - jnp.arange(shard_len + 3)
        picked = jnp.take(long_filt, jnp.clip(lag_pos, 0, sp_size * shard_len - 1), axis=2)
        parts = []
        for layer_idx in range(NUM_LAYERS):
            for which, cache in ((0, v_cache), (1, z_cache)):
                rows = cache[layer_idx].astype(f32)
                parts.append(jnp.stack([
                    jnp.sum(rows * picked[layer_idx, which, 3 - j:3 - j + shard_len][None], axis=1)
                    for j in range(NUM_STEPS)]))
        part = lax.psum_scatter(jnp.stack(parts), "sp", scatter_dimension=2, tiled=True)
        part = part.reshape(NUM_LAYERS, 2, NUM_STEPS, own, -1)
        hidden = lax.dynamic_slice_in_dim(step_emb, sp_idx * own, own, axis=1).astype(f32)
        state_own = lax.dynamic_slice_in_dim(short_state, sp_idx * own, own, axis=1)
        v_rows, z_rows, p_rows = [], [], []
        for layer_idx in range(NUM_LAYERS):
            normed = layer_norm(hidden).astype(jnp.bfloat16)
            proj = jnp.einsum("jbd,dgc->jbgc", normed, w_in[layer_idx], preferred_element_type=f32)
            proj = (proj + b_in[layer_idx]).astype(jnp.bfloat16)
            p_rows.append(proj[NUM_STEPS - 2:])
            prev = jnp.moveaxis(state_own[layer_idx], 1, 0)
            ext = jnp.concatenate([prev, proj], axis=0).astype(f32)
            taps = short_taps[layer_idx]
            mixed = taps[0] * ext[2:] + taps[1] * ext[1:-1] + taps[2] * ext[:-2]

            def conv(which, new_rows):
                filt = long_filt[layer_idx, which]
                outs = []
                for j in range(NUM_STEPS):
                    acc = part[layer_idx, which, j]
                    for i in range(j + 1):
                        acc = acc + filt[j - i] * new_rows[i]
                    outs.append(acc + skip_gain[layer_idx, which] * new_rows[j])
                return jnp.stack(outs)

            v_new = mixed[:, :, 2].astype(jnp.bfloat16).astype(f32)
            z_new = (mixed[:, :, 0] * conv(0, v_new)).astype(jnp.bfloat16).astype(f32)
            y_new = (mixed[:, :, 1] * conv(1, z_new)).astype(jnp.bfloat16)
            v_rows.append(v_new)
            z_rows.append(z_new)
            hidden = hidden + lax.psum(jnp.dot(y_new, w_out[layer_idx], preferred_element_type=f32), "tp") + b_out[layer_idx]
            inner = jax.nn.gelu(jnp.dot(layer_norm(hidden).astype(jnp.bfloat16), w_up[layer_idx], preferred_element_type=f32)).astype(jnp.bfloat16)
            hidden = hidden + lax.psum(jnp.dot(inner, w_down[layer_idx], preferred_element_type=f32), "tp")
        zero = jnp.minimum(jnp.abs(b_out[0, 0]), 0.0)
        hidden_all = gather_rows(hidden, 1, zero)
        vz = gather_rows(jnp.stack([jnp.stack(v_rows), jnp.stack(z_rows)]), 3, zero)
        vz = jnp.swapaxes(vz, 2, 3).astype(jnp.bfloat16)
        p_all = gather_rows(jnp.stack(p_rows), 2, zero)
        states = jnp.swapaxes(p_all, 1, 2).astype(jnp.bfloat16)
        last = sp_idx * shard_len == start_pos

        def put(cache, new):
            old = cache[:, :, :NUM_STEPS]
            return lax.dynamic_update_slice(cache, jnp.where(last, new, old), (0, 0, 0, 0))

        return (hidden_all, put(v_cache, vz[0]), put(z_cache, vz[1]), states)

    specs_in = (
        P(None, "dp", None),
        P(None, "dp", "sp", "tp"),
        P(None, "dp", "sp", "tp"),
        P(None, "dp", None, None, "tp"),
        P(None, None, None, "tp"),
        P(None, None, "tp"),
        P(None, None, None, "tp"),
        P(None, None, None, "tp"),
        P(None, None, "tp"),
        P(None, "tp", None),
        P(None, None),
        P(None, None, "tp"),
        P(None, "tp", None),
    )
    specs_out = (
        P(None, "dp", None),
        P(None, "dp", "sp", "tp"),
        P(None, "dp", "sp", "tp"),
        P(None, "dp", None, None, "tp"),
    )
    return jax.shard_map(device_fn, mesh=mesh, in_specs=specs_in, out_specs=specs_out, check_vma=False)
```

```python
import jax
import jax.numpy as jnp
from jax import lax
from jax.experimental import pallas as pl
from jax.experimental.pallas import tpu as pltpu
from jax.sharding import PartitionSpec as P

NUM_STEPS = 4
NUM_LAYERS = 2
MESH = pl.DeviceIdType.MESH
F32 = jnp.float32
BF16 = jnp.bfloat16
VMEM_LIMIT = 66_500_000


def conv_kernel(shape, v_ref, z_ref, f_ref, vo_ref, zo_ref, part_ref, buf, fwin, fsh, rsem, wsem, fsem):
    num_seq, shard_len, chan, start_pos = shape
    half = num_seq // 2
    own = num_seq // 4
    shard_start = lax.axis_index("sp") * shard_len
    base = pl.multiple_of(jnp.maximum(start_pos - shard_len - shard_start, 0), 8)
    window = shard_len + 8

    filt_copies, reads, writes = [], [], []
    for a in range(4):
        layer, which = divmod(a, 2)
        src = (v_ref, z_ref)[which]
        dst = (vo_ref, zo_ref)[which]
        filt_copies.append(pltpu.make_async_copy(f_ref.at[layer, which, pl.ds(base, window)], fwin.at[a], fsem.at[a]))
        for c in range(2):
            reads.append(pltpu.make_async_copy(src.at[layer, pl.ds(c * half, half)], buf.at[a, c], rsem.at[a, c]))
            writes.append(pltpu.make_async_copy(buf.at[a, c], dst.at[layer, pl.ds(c * half, half)], wsem.at[a, c]))
    for a in range(4):
        filt_copies[a].start()
        reads[2 * a].start()
        reads[2 * a + 1].start()

    sub = lax.broadcasted_iota(jnp.int32, (8, chan), 0)

    def rev8(x):
        x = pltpu.roll(x, 4, 0)
        x = jnp.where((sub // 2) % 2 == 0, pltpu.roll(x, 6, 0), pltpu.roll(x, 2, 0))
        return jnp.where(sub % 2 == 0, pltpu.roll(x, 7, 0), pltpu.roll(x, 1, 0))

    groups = shard_len // 8
    for a in range(4):
        filt_copies[a].wait()

        def prep(g, prev):
            cur = rev8(fwin[a, pl.ds(pl.multiple_of((groups - 1 - g) * 8, 8), 8), :])
            for j in range(NUM_STEPS):
                mixed = jnp.where(sub >= 7 - j, prev, cur)
                fsh[j, pl.ds(pl.multiple_of(g * 8, 8), 8), :] = pltpu.roll(mixed, j + 1, 0)
            return cur

        lax.fori_loop(0, groups, prep, rev8(fwin[a, pl.ds(groups * 8, 8), :]))
        for c in range(2):
            reads[2 * a + c].wait()
            writes[2 * a + c].start()

            def lanes_body(lc, carry):
                lanes = pl.ds(pl.multiple_of(lc * 128, 128), 128)

                def body(g, accs):
                    rows = pl.ds(pl.multiple_of(g * 16, 16), 16)
                    filts = [fsh[j, rows, lanes] for j in range(NUM_STEPS)]
                    out = []
                    for b in range(half):
                        v = buf[a, c, b, rows, lanes].astype(F32)
                        for j in range(NUM_STEPS):
                            m = v * filts[j]
                            out.append(accs[b * NUM_STEPS + j] + m[:8] + m[8:])
                    return tuple(out)

                zero = jnp.zeros((8, 128), F32)
                accs = lax.fori_loop(0, shard_len // 16, body, (zero,) * (half * NUM_STEPS))
                for b in range(half):
                    for j in range(NUM_STEPS):
                        row = j * own + b % own
                        part_ref[a, c * (half // own) + b // own, row:row + 1, lanes] = jnp.sum(
                            accs[b * NUM_STEPS + j], axis=0, keepdims=True)
                return carry

            lax.fori_loop(0, chan // 128, lanes_body, 0)
    for copy in writes:
        copy.wait()


def dense_kernel(emb_ref, part_ref, state_ref, b_in_ref, taps_ref, skip_ref, b_out_ref, f_ref, w_in_ref, w_out_ref, w_up_ref, w_down_ref,
                 hid_ref, vzp_ref,
                 w_in, w_out, w_up, w_down, lags, ext, shifted, xrow, inner,
                 part_in, rs_out, rs_in, hid, fin, vzp,
                 in_sem, lag_sem, out_sem, up_sem, down_sem,
                 part_send, part_recv, rs_send, rs_recv, ag_send, ag_recv, fin_send, fin_recv, vzp_send, vzp_recv):
    t = lax.axis_index("tp")
    s = lax.axis_index("sp")
    flip_t = (3 - t, (t + 2) % 4, t + 1 - 2 * (t % 2))
    flip_s = (3 - s, (s + 2) % 4, s + 1 - 2 * (s % 2))
    rows = NUM_STEPS * 4
    cols = ext.shape[-1]
    dim = 4 * cols

    in_copies = [[pltpu.make_async_copy(w_in_ref.at[l, g], w_in.at[l, g], in_sem.at[l, g]) for g in range(3)] for l in range(2)]
    out_copies = [[pltpu.make_async_copy(w_out_ref.at[l, pl.ds(256 * i, 256)], w_out.at[l, pl.ds(256 * i, 256)], out_sem.at[l, i])
                   for i in range(cols // 256)] for l in range(2)]
    up_copies = [[pltpu.make_async_copy(w_up_ref.at[l, pl.ds(512 * i, 512)], w_up.at[l, pl.ds(512 * i, 512)], up_sem.at[l, i])
                  for i in range(4)] for l in range(2)]
    down_copies = [[pltpu.make_async_copy(w_down_ref.at[l, pl.ds(512 * i, 512)], w_down.at[l, pl.ds(512 * i, 512)], down_sem.at[l, i])
                    for i in range(4)] for l in range(2)]
    lag_copy = pltpu.make_async_copy(f_ref.at[:, :, pl.ds(0, 8)], lags, lag_sem)

    def start(copies):
        for copy in copies:
            copy.start()

    def wait(copies):
        for copy in copies:
            copy.wait()

    start(in_copies[0])
    lag_copy.start()
    start(out_copies[0])

    barrier = pltpu.get_barrier_semaphore()
    for k in range(3):
        pl.semaphore_signal(barrier, inc=1, device_id={"tp": flip_t[k]}, device_id_type=MESH)
        pl.semaphore_signal(barrier, inc=1, device_id={"sp": flip_s[k]}, device_id_type=MESH)
    pl.semaphore_wait(barrier, 6)

    sends = []

    def send(src, dst, send_sem, recv_sem, device_id):
        copy = pltpu.make_async_remote_copy(src_ref=src, dst_ref=dst, send_sem=send_sem, recv_sem=recv_sem,
                                            device_id=device_id, device_id_type=MESH)
        copy.start()
        sends.append(copy)
        return copy

    part_copies = [[send(part_ref.at[a, flip_s[k]], part_in.at[a, k], part_send.at[a, k], part_recv.at[a, k], {"sp": flip_s[k]})
                    for k in range(3)] for a in range(4)]

    def norm_to_xrow(chunks):
        mean = sum(jnp.sum(c, axis=-1, keepdims=True) for c in chunks) / dim
        cent = [c - mean for c in chunks]
        var = sum(jnp.sum(c * c, axis=-1, keepdims=True) for c in cent) / dim
        scale = lax.rsqrt(var + 1e-5)
        for i, c in enumerate(cent):
            xrow[:, cols * i:cols * (i + 1)] = (c * scale).astype(BF16)

    def reduce_chunks(r, chunk_of, base_ref, bias_row):
        copies = []
        for k in range(3):
            rs_out[r, k] = chunk_of(flip_t[k])
            copies.append(send(rs_out.at[r, k], rs_in.at[r, k], rs_send.at[r, k], rs_recv.at[r, k], {"tp": flip_t[k]}))
        total = base_ref[t] + chunk_of(t)
        if bias_row is not None:
            total = total + bias_row
        for k in (2, 1, 0):
            copies[k].wait_recv()
            total = total + rs_in[r, k]
        return total

    def gather_chunks(r, total):
        hid[r, t] = total
        copies = [send(hid.at[r, t], hid.at[r, t], ag_send.at[r, k], ag_recv.at[r, k], {"tp": flip_t[k]}) for k in range(3)]
        for copy in copies:
            copy.wait_recv()

    shifted[0:rows, :] = jnp.zeros((rows, cols), F32)
    for l in range(NUM_LAYERS):
        base = emb_ref if l == 0 else hid.at[2 * l - 1]
        norm_to_xrow([base[i] for i in range(4)])
        x = xrow[...]
        for g in range(3):
            in_copies[l][g].wait()
            proj = jnp.dot(x, w_in[l, g], preferred_element_type=F32) + b_in_ref[g, l:l + 1]
            proj = proj.astype(BF16).astype(F32)
            ext[g, 0:8] = state_ref[l, g]
            ext[g, 8:24] = proj
            vzp[s, l, 8 * g:8 * g + 8] = proj[8:16]
        start(up_copies[l])
        start(down_copies[l])

        def mixed(g):
            return (taps_ref[0, g, l:l + 1] * ext[g, 8:24] + taps_ref[1, g, l:l + 1] * ext[g, 4:20]
                    + taps_ref[2, g, l:l + 1] * ext[g, 0:16])

        def conv(which, new):
            a = 2 * l + which
            if a == 0:
                lag_copy.wait()
            shifted[rows:2 * rows, :] = new
            acc = skip_ref[l, which:which + 1] * new
            for d in range(NUM_STEPS):
                acc = acc + lags[l, which, d:d + 1] * shifted[rows - 4 * d:2 * rows - 4 * d]
            acc = acc + part_ref[a, s]
            for k in range(3):
                part_copies[a][k].wait_recv()
                acc = acc + part_in[a, k]
            return acc

        v_new = mixed(2).astype(BF16).astype(F32)
        vzp[s, l, 24:40] = v_new
        z_new = (mixed(0) * conv(0, v_new)).astype(BF16).astype(F32)
        vzp[s, l, 40:56] = z_new
        y = (mixed(1) * conv(1, z_new)).astype(BF16)
        wait(out_copies[l])
        total = reduce_chunks(
            2 * l, lambda c: jnp.dot(y, w_out[l, :, pl.ds(pl.multiple_of(c * cols, cols), cols)], preferred_element_type=F32),
            base, b_out_ref[l, t])
        gather_chunks(2 * l, total)
        vzp_copies = [send(vzp.at[s, l], vzp.at[s, l], vzp_send.at[l, k], vzp_recv.at[l, k], {"sp": flip_s[k]}) for k in range(3)]
        if l == 0:
            first_vzp = vzp_copies
            start(in_copies[1])
            start(out_copies[1])
        norm_to_xrow([hid[2 * l, i] for i in range(4)])
        x = xrow[...]
        wait(up_copies[l])
        for i in range(4):
            up = jnp.dot(x, w_up[l, :, cols * i:cols * (i + 1)], preferred_element_type=F32)
            inner[:, cols * i:cols * (i + 1)] = jax.nn.gelu(up).astype(BF16)
        act = inner[...]
        wait(down_copies[l])
        total = reduce_chunks(
            2 * l + 1, lambda c: jnp.dot(act, w_down[l, :, pl.ds(pl.multiple_of(c * cols, cols), cols)], preferred_element_type=F32),
            hid.at[2 * l], None)
        if l == 0:
            gather_chunks(1, total)

    fin[s, t] = total
    chunk_ids = (t,) + flip_t
    tp_copies = [send(fin.at[s, t], fin.at[s, t], ag_send.at[3, k], ag_recv.at[3, k], {"tp": flip_t[k]}) for k in range(3)]
    fin_copies = []
    for i in (0, 3, 2, 1):
        if i > 0:
            tp_copies[i - 1].wait_recv()
        for k in (2, 1, 0):
            chunk = fin.at[s, chunk_ids[i]]
            fin_copies.append(send(chunk, chunk, fin_send.at[i, k], fin_recv.at[i, k], {"sp": flip_s[k]}))
    for copy in fin_copies:
        copy.wait_recv()
    for g in range(4):
        for i in range(4):
            for j in range(NUM_STEPS):
                hid_ref[j, 4 * g:4 * g + 4, cols * i:cols * (i + 1)] = fin[g, i, 4 * j:4 * j + 4]
    for copy in first_vzp + vzp_copies:
        copy.wait_recv()
    vzp_ref[...] = vzp[...]
    for copy in sends:
        copy.wait_send()


def solution(mesh):
    sp_size = mesh.shape["sp"]

    def device_fn(step_emb, v_cache, z_cache, short_state, w_in, b_in, short_taps, long_filt, skip_gain, w_out, b_out, w_up, w_down):
        num_seq, shard_len, chan = v_cache.shape[1:]
        dim = step_emb.shape[-1]
        start_pos = shard_len * sp_size * 3 // 4
        sp_idx = lax.axis_index("sp")
        own = num_seq // sp_size
        rows = NUM_STEPS * own
        hbm = pl.BlockSpec(memory_space=pl.ANY)
        vmem = pl.BlockSpec(memory_space=pltpu.VMEM)
        sds = jax.ShapeDtypeStruct

        v_out, z_out, part = pl.pallas_call(
            lambda *refs: conv_kernel((num_seq, shard_len, chan, start_pos), *refs),
            name="conv_kernel",
            out_shape=(sds(v_cache.shape, BF16), sds(z_cache.shape, BF16), sds((4, sp_size, rows, chan), F32)),
            in_specs=[hbm] * 3,
            out_specs=(hbm, hbm, vmem),
            scratch_shapes=[
                pltpu.VMEM((4, 2, num_seq // 2, shard_len, chan), BF16),
                pltpu.VMEM((4, shard_len + 8, chan), F32),
                pltpu.VMEM((NUM_STEPS, shard_len, chan), F32),
                pltpu.SemaphoreType.DMA((4, 2)),
                pltpu.SemaphoreType.DMA((4, 2)),
                pltpu.SemaphoreType.DMA((4,)),
            ],
            compiler_params=pltpu.CompilerParams(vmem_limit_bytes=40_000_000),
        )(v_cache, z_cache, long_filt)

        emb = lax.dynamic_slice_in_dim(step_emb, sp_idx * own, own, axis=1).astype(F32)
        emb = jnp.moveaxis(emb.reshape(rows, 4, chan), 1, 0)
        state = lax.dynamic_slice_in_dim(short_state, sp_idx * own, own, axis=1).astype(F32)
        state = jnp.transpose(state, (0, 3, 2, 1, 4)).reshape(NUM_LAYERS, 3, 2 * own, chan)
        dma = pltpu.SemaphoreType.DMA
        chunk = (rows, chan)
        hidden, vzp = pl.pallas_call(
            dense_kernel,
            name="dense_kernel",
            out_shape=(sds((NUM_STEPS, num_seq, dim), F32), sds((sp_size, NUM_LAYERS, 56, chan), F32)),
            in_specs=[vmem] * 7 + [hbm] * 5,
            out_specs=(vmem, vmem),
            scratch_shapes=[
                pltpu.VMEM((2, 3, dim, chan), BF16),
                pltpu.VMEM((2, chan, dim), BF16),
                pltpu.VMEM((2, dim, w_up.shape[-1]), BF16),
                pltpu.VMEM((2, w_down.shape[1], dim), BF16),
                pltpu.VMEM((2, 2, 8, chan), F32),
                pltpu.VMEM((3, rows + 8, chan), F32),
                pltpu.VMEM((2 * rows, chan), F32),
                pltpu.VMEM((rows, dim), BF16),
                pltpu.VMEM((rows, w_up.shape[-1]), BF16),
                pltpu.VMEM((4, 3) + chunk, F32),
                pltpu.VMEM((4, 3) + chunk, F32),
                pltpu.VMEM((4, 3) + chunk, F32),
                pltpu.VMEM((3, 4) + chunk, F32),
                pltpu.VMEM((4, 4) + chunk, F32),
                pltpu.VMEM((4, 2, 56, chan), F32),
                dma((2, 3)), dma(()), dma((2, 2)), dma((2, 4)), dma((2, 4)),
                dma((4, 3)), dma((4, 3)), dma((4, 3)), dma((4, 3)), dma((4, 3)), dma((4, 3)), dma((4, 3)), dma((4, 3)),
                dma((2, 3)), dma((2, 3)),
            ],
            compiler_params=pltpu.CompilerParams(collective_id=0, has_side_effects=True, vmem_limit_bytes=VMEM_LIMIT),
        )(emb, part, state, jnp.transpose(b_in, (1, 0, 2)), jnp.transpose(short_taps, (1, 2, 0, 3)), skip_gain,
          b_out.reshape(NUM_LAYERS, 4, 1, chan), long_filt, jnp.transpose(w_in, (0, 2, 1, 3)), w_out, w_up, w_down)

        p_rows = vzp[:, :, :24].reshape(sp_size, NUM_LAYERS, 3, 2, own, chan)
        states = jnp.transpose(p_rows, (1, 0, 4, 3, 2, 5)).reshape(short_state.shape).astype(BF16)
        last = sp_idx * shard_len == start_pos

        def put(cache, new):
            new = new.reshape(sp_size, NUM_LAYERS, NUM_STEPS, own, chan)
            new = jnp.transpose(new, (1, 0, 3, 2, 4)).reshape(NUM_LAYERS, num_seq, NUM_STEPS, chan).astype(BF16)
            old = cache[:, :, :NUM_STEPS]
            return lax.dynamic_update_slice(cache, jnp.where(last, new, old), (0, 0, 0, 0))

        return (hidden, put(v_out, vzp[:, :, 24:40]), put(z_out, vzp[:, :, 40:56]), states)

    specs_in = (
        P(None, "dp", None),
        P(None, "dp", "sp", "tp"),
        P(None, "dp", "sp", "tp"),
        P(None, "dp", None, None, "tp"),
        P(None, None, None, "tp"),
        P(None, None, "tp"),
        P(None, None, None, "tp"),
        P(None, None, None, "tp"),
        P(None, None, "tp"),
        P(None, "tp", None),
        P(None, None),
        P(None, None, "tp"),
        P(None, "tp", None),
    )
    specs_out = (
        P(None, "dp", None),
        P(None, "dp", "sp", "tp"),
        P(None, "dp", "sp", "tp"),
        P(None, "dp", None, None, "tp"),
    )
    return jax.shard_map(device_fn, mesh=mesh, in_specs=specs_in, out_specs=specs_out, check_vma=False)
```

```python
import jax
import jax.numpy as jnp
from jax import lax
from jax.experimental import pallas as pl
from jax.experimental.pallas import tpu as pltpu
from jax.sharding import PartitionSpec as P

NUM_STEPS = 4
NUM_LAYERS = 2
MESH = pl.DeviceIdType.MESH
F32 = jnp.float32
BF16 = jnp.bfloat16
VMEM_LIMIT = 66_500_000


def shift_filters(fwin, fsh):
    groups = fsh.shape[1] // 8
    sub = lax.broadcasted_iota(jnp.int32, (8, fsh.shape[2]), 0)

    def prep(g, prev):
        cur = fwin[pl.ds(pl.multiple_of((groups - 1 - g) * 8, 8), 8), :]
        for j in range(NUM_STEPS):
            mixed = jnp.where(sub <= j, prev, cur)
            fsh[j, pl.ds(pl.multiple_of(g * 8, 8), 8), :] = jnp.take_along_axis(mixed, (j - sub) % 8, axis=0)
        return cur

    lax.fori_loop(0, groups, prep, fwin[pl.ds(groups * 8, 8), :])


def conv_unit(buf, fsh, out):
    own, shard_len, chan = buf.shape

    def block_body(i, carry):
        lanes = pl.ds(pl.multiple_of(i * 128, 128), 128)
        accs = [jnp.zeros((8, 128), F32)] * (own * NUM_STEPS)
        for g in range(shard_len // 16):
            rows = pl.ds(g * 16, 16)
            filts = [fsh[j, rows, lanes] for j in range(NUM_STEPS)]
            for b in range(own):
                v = buf[b, rows, lanes].astype(F32)
                for j in range(NUM_STEPS):
                    m = v * filts[j]
                    accs[j * own + b] = accs[j * own + b] + m[:8] + m[8:]
        for row in range(own * NUM_STEPS):
            out[row:row + 1, lanes] = jnp.sum(accs[row], axis=0, keepdims=True)
        return carry

    lax.fori_loop(0, chan // 128, block_body, 0)


def window_base(shard_len):
    return pl.multiple_of(jnp.maximum((2 - lax.axis_index("sp")) * shard_len, 0), 8)


def conv_kernel(v_ref, z_ref, f_ref, vo_ref, zo_ref, part_ref, buf, fwin, fsh, rsem, wsem, fsem):
    shard_len = v_ref.shape[2]
    base = window_base(shard_len)
    filt_copies = [pltpu.make_async_copy(f_ref.at[0, a, pl.ds(base, shard_len + 8)], fwin.at[a], fsem.at[a]) for a in range(2)]
    order = []
    for i in range(8):
        order += [(0, i // 4, i % 4), (1, i // 4, i % 4)]
    reads = [pltpu.make_async_copy((v_ref, z_ref)[a].at[layer, pl.ds(4 * q, 4)], buf.at[n], rsem.at[n])
             for n, (layer, a, q) in enumerate(order)]
    writes = [pltpu.make_async_copy(buf.at[n], (vo_ref, zo_ref)[a].at[layer, pl.ds(4 * q, 4)], wsem.at[n])
              for n, (layer, a, q) in enumerate(order)]
    filt_copies[0].start()
    for n in range(4):
        reads[n].start()
    filt_copies[1].start()
    for n, (layer, a, q) in enumerate(order):
        if layer == 0 and q == 0:
            filt_copies[a].wait()
            shift_filters(fwin.at[a], fsh)
        reads[n].wait()
        writes[n].start()
        if n + 4 < 16:
            reads[n + 4].start()
        if layer == 1:
            conv_unit(buf.at[n - 1], fsh, part_ref.at[a, q])
    for copy in writes:
        copy.wait()


def dense_kernel(emb_ref, state_ref, b_in_ref, taps_ref, skip_ref, b_out_ref, part_hbm, v_ref, z_ref, f_ref, w_in_ref, w_out_ref, w_up_ref, w_down_ref,
                 fin_ref, vzp_ref,
                 w_in, w_out, w_up, w_down, lags, ext, shifted, xrow, inner, emb,
                 buf, fwin, fsh, part_ref, part_in, rs_out, rs_in, hid, fin, vzp,
                 in_sem, lag_sem, out_sem, up_sem, down_sem, own_sem, buf_sem, fwin_sem,
                 part_send, part_recv, rs_send, rs_recv, ag_send, ag_recv, fin_send, fin_recv, vzp_send, vzp_recv):
    t = lax.axis_index("tp")
    s = lax.axis_index("sp")
    flip_t = (3 - t, (t + 2) % 4, t + 1 - 2 * (t % 2))
    flip_s = (3 - s, (s + 2) % 4, s + 1 - 2 * (s % 2))
    rows = NUM_STEPS * 4
    cols = ext.shape[-1]
    dim = 4 * cols

    in_copies = [[pltpu.make_async_copy(w_in_ref.at[l, g], w_in.at[l, g], in_sem.at[l, g]) for g in range(3)] for l in range(2)]
    out_copies = [[pltpu.make_async_copy(w_out_ref.at[l, pl.ds(256 * i, 256)], w_out.at[l, pl.ds(256 * i, 256)], out_sem.at[l, i])
                   for i in range(cols // 256)] for l in range(2)]
    up_copies = [[pltpu.make_async_copy(w_up_ref.at[l, pl.ds(512 * i, 512)], w_up.at[l, pl.ds(512 * i, 512)], up_sem.at[l, i])
                  for i in range(4)] for l in range(2)]
    down_copies = [[pltpu.make_async_copy(w_down_ref.at[l, pl.ds(512 * i, 512)], w_down.at[l, pl.ds(512 * i, 512)], down_sem.at[l, i])
                    for i in range(4)] for l in range(2)]
    lag_copy = pltpu.make_async_copy(f_ref.at[:, :, pl.ds(0, 8)], lags, lag_sem)

    def start(copies):
        for copy in copies:
            copy.start()

    def wait(copies):
        for copy in copies:
            copy.wait()

    part_copy = pltpu.make_async_copy(part_hbm, part_ref.at[pl.ds(0, 2)], own_sem)
    shard_len = v_ref.shape[2]
    fwin_copies = [pltpu.make_async_copy(f_ref.at[1, a, pl.ds(window_base(shard_len), shard_len + 8)], fwin.at[a], fwin_sem.at[a])
                   for a in range(2)]
    reads = [pltpu.make_async_copy((v_ref, z_ref)[n // 4].at[1, pl.ds(4 * (n % 4), 4)], buf.at[n % 4], buf_sem.at[n]) for n in range(8)]
    part_copy.start()
    start(in_copies[0])
    lag_copy.start()
    start(out_copies[0])

    barrier = pltpu.get_barrier_semaphore()
    for k in range(3):
        pl.semaphore_signal(barrier, inc=1, device_id={"tp": flip_t[k]}, device_id_type=MESH)
        pl.semaphore_signal(barrier, inc=1, device_id={"sp": flip_s[k]}, device_id_type=MESH)
    pl.semaphore_wait(barrier, 6)

    for k in range(4):
        @pl.when(s == k)
        def _():
            for j in range(NUM_STEPS):
                for i in range(4):
                    emb[i, 4 * j:4 * j + 4] = emb_ref[j, :, cols * i:cols * (i + 1)].astype(F32)[4 * k:4 * k + 4]

    sends = []

    def send(src, dst, send_sem, recv_sem, device_id):
        copy = pltpu.make_async_remote_copy(src_ref=src, dst_ref=dst, send_sem=send_sem, recv_sem=recv_sem,
                                            device_id=device_id, device_id_type=MESH)
        copy.start()
        sends.append(copy)
        return copy

    part_copy.wait()
    def send_part(a):
        return [send(part_ref.at[a, flip_s[k]], part_in.at[a, k], part_send.at[a, k], part_recv.at[a, k], {"sp": flip_s[k]})
                for k in range(3)]

    part_copies = [send_part(0), send_part(1), None, None]

    def cached_terms(a):
        fwin_copies[a].wait()
        shift_filters(fwin.at[a], fsh)
        for q in range(4):
            n = 4 * a + q
            reads[n].wait()
            conv_unit(buf.at[q], fsh, part_ref.at[2 + a, q])
            if n + 4 < 8:
                reads[n + 4].start()
        part_copies[2 + a] = send_part(2 + a)

    def norm_to_xrow(chunks):
        mean = sum(jnp.sum(c, axis=-1, keepdims=True) for c in chunks) / dim
        cent = [c - mean for c in chunks]
        var = sum(jnp.sum(c * c, axis=-1, keepdims=True) for c in cent) / dim
        scale = lax.rsqrt(var + 1e-5)
        for i, c in enumerate(cent):
            xrow[:, cols * i:cols * (i + 1)] = (c * scale).astype(BF16)

    def reduce_chunks(r, chunk_of, base_ref, bias_row):
        copies = []
        for k in range(3):
            rs_out[r, k] = chunk_of(flip_t[k])
            copies.append(send(rs_out.at[r, k], rs_in.at[r, k], rs_send.at[r, k], rs_recv.at[r, k], {"tp": flip_t[k]}))
        total = base_ref[t] + chunk_of(t)
        if r == 0:
            cached_terms(0)
        if bias_row is not None:
            total = total + bias_row
        for k in (2, 1, 0):
            copies[k].wait_recv()
            total = total + rs_in[r, k]
        return total

    def gather_chunks(r, total):
        hid[r, t] = total
        copies = [send(hid.at[r, t], hid.at[r, t], ag_send.at[r, k], ag_recv.at[r, k], {"tp": flip_t[k]}) for k in range(3)]
        if r == 0:
            cached_terms(1)
        for copy in copies:
            copy.wait_recv()

    shifted[0:rows, :] = jnp.zeros((rows, cols), F32)
    for l in range(NUM_LAYERS):
        base = emb if l == 0 else hid.at[2 * l - 1]
        norm_to_xrow([base[i] for i in range(4)])
        x = xrow[...]
        for g in range(3):
            in_copies[l][g].wait()
            proj = jnp.dot(x, w_in[l, g], preferred_element_type=F32) + b_in_ref[g, l:l + 1]
            proj = proj.astype(BF16).astype(F32)
            ext[g, 8:24] = proj
            for b in range(4):
                old = state_ref[l, 4 * s + b, g].astype(F32)
                ext[g, b:b + 1] = old[0:1]
                ext[g, 4 + b:5 + b] = old[1:2]
            vzp[s, l, 8 * g:8 * g + 8] = proj[8:16]
        if l == 0:
            start(fwin_copies)
            start(reads[:4])
        start(up_copies[l])
        start(down_copies[l])

        def mixed(g):
            return (taps_ref[0, g, l:l + 1] * ext[g, 8:24] + taps_ref[1, g, l:l + 1] * ext[g, 4:20]
                    + taps_ref[2, g, l:l + 1] * ext[g, 0:16])

        def conv(which, new):
            a = 2 * l + which
            if a == 0:
                lag_copy.wait()
            shifted[rows:2 * rows, :] = new
            acc = skip_ref[l, which:which + 1] * new
            for d in range(NUM_STEPS):
                acc = acc + lags[l, which, d:d + 1] * shifted[rows - 4 * d:2 * rows - 4 * d]
            acc = acc + part_ref[a, s]
            for k in range(3):
                part_copies[a][k].wait_recv()
                acc = acc + part_in[a, k]
            return acc

        v_new = mixed(2).astype(BF16).astype(F32)
        vzp[s, l, 24:40] = v_new
        z_new = (mixed(0) * conv(0, v_new)).astype(BF16).astype(F32)
        vzp[s, l, 40:56] = z_new
        y = (mixed(1) * conv(1, z_new)).astype(BF16)
        wait(out_copies[l])
        total = reduce_chunks(
            2 * l, lambda c: jnp.dot(y, w_out[l, :, pl.ds(pl.multiple_of(c * cols, cols), cols)], preferred_element_type=F32),
            base, b_out_ref[l:l + 1, pl.ds(pl.multiple_of(t * cols, cols), cols)])
        gather_chunks(2 * l, total)
        vzp_copies = [send(vzp.at[s, l], vzp.at[s, l], vzp_send.at[l, k], vzp_recv.at[l, k], {"sp": flip_s[k]}) for k in range(3)]
        if l == 0:
            first_vzp = vzp_copies
            start(in_copies[1])
            start(out_copies[1])
        norm_to_xrow([hid[2 * l, i] for i in range(4)])
        x = xrow[...]
        wait(up_copies[l])
        for i in range(4):
            up = jnp.dot(x, w_up[l, :, cols * i:cols * (i + 1)], preferred_element_type=F32)
            inner[:, cols * i:cols * (i + 1)] = jax.nn.gelu(up).astype(BF16)
        act = inner[...]
        wait(down_copies[l])
        total = reduce_chunks(
            2 * l + 1, lambda c: jnp.dot(act, w_down[l, :, pl.ds(pl.multiple_of(c * cols, cols), cols)], preferred_element_type=F32),
            hid.at[2 * l], None)
        if l == 0:
            gather_chunks(1, total)

    fin[s, t] = total
    chunk_ids = (t,) + flip_t
    tp_copies = [send(fin.at[s, t], fin.at[s, t], ag_send.at[3, k], ag_recv.at[3, k], {"tp": flip_t[k]}) for k in range(3)]
    fin_copies = []
    for i in (0, 3, 2, 1):
        if i > 0:
            tp_copies[i - 1].wait_recv()
        for k in (2, 1, 0):
            chunk = fin.at[s, chunk_ids[i]]
            fin_copies.append(send(chunk, chunk, fin_send.at[i, k], fin_recv.at[i, k], {"sp": flip_s[k]}))
    for copy in fin_copies:
        copy.wait_recv()
    fin_out = pltpu.make_async_copy(fin, fin_ref, own_sem)
    fin_out.start()
    for copy in first_vzp + vzp_copies:
        copy.wait_recv()
    vzp_out = pltpu.make_async_copy(vzp, vzp_ref, lag_sem)
    vzp_out.start()
    fin_out.wait()
    vzp_out.wait()
    for copy in sends:
        copy.wait_send()


def finish_kernel(fin_ref, vzp_ref, v_ref, z_ref, hid_ref, state_ref, vo_ref, zo_ref, new_rows, sem):
    cols = fin_ref.shape[-1]
    last = lax.axis_index("sp") == 3

    @pl.when(last)
    def _():
        new_rows[...] = jnp.zeros_like(new_rows)
        for a in range(2):
            for l in range(NUM_LAYERS):
                for g in range(4):
                    for b in range(4):
                        for j in range(NUM_STEPS):
                            row = 24 + 16 * a + 4 * j + b
                            new_rows[a, l, 4 * g + b, j:j + 1] = vzp_ref[g, l, row:row + 1].astype(BF16)
        for a, dst in enumerate((vo_ref, zo_ref)):
            pltpu.make_async_copy(new_rows.at[a], dst.at[:, :, pl.ds(0, 8)], sem.at[a]).start()

    for g in range(4):
        for i in range(4):
            for j in range(NUM_STEPS):
                hid_ref[j, 4 * g:4 * g + 4, cols * i:cols * (i + 1)] = fin_ref[g, i, 4 * j:4 * j + 4]
        for l in range(NUM_LAYERS):
            for c in range(3):
                for b in range(4):
                    pair = jnp.concatenate([vzp_ref[g, l, 8 * c + b:8 * c + b + 1], vzp_ref[g, l, 8 * c + 4 + b:8 * c + 5 + b]], axis=0)
                    state_ref[l, 4 * g + b, c] = pair.astype(BF16)

    @pl.when(last)
    def _():
        for a, dst in enumerate((vo_ref, zo_ref)):
            pltpu.make_async_copy(new_rows.at[a], dst.at[:, :, pl.ds(0, 8)], sem.at[a]).wait()


def solution(mesh):
    sp_size = mesh.shape["sp"]

    def device_fn(step_emb, v_cache, z_cache, short_state, w_in, b_in, short_taps, long_filt, skip_gain, w_out, b_out, w_up, w_down):
        num_seq, shard_len, chan = v_cache.shape[1:]
        dim = step_emb.shape[-1]
        own = num_seq // sp_size
        rows = NUM_STEPS * own
        hbm = pl.BlockSpec(memory_space=pl.ANY)
        vmem = pl.BlockSpec(memory_space=pltpu.VMEM)
        sds = jax.ShapeDtypeStruct

        v_out, z_out, part = pl.pallas_call(
            conv_kernel,
            name="conv_kernel",
            out_shape=(sds(v_cache.shape, BF16), sds(z_cache.shape, BF16), sds((2, sp_size, rows, chan), F32)),
            in_specs=[hbm] * 3,
            out_specs=(hbm, hbm, vmem),
            scratch_shapes=[
                pltpu.VMEM((16, own, shard_len, chan), BF16),
                pltpu.VMEM((2, shard_len + 8, chan), F32),
                pltpu.VMEM((NUM_STEPS, shard_len, chan), F32),
                pltpu.SemaphoreType.DMA((16,)),
                pltpu.SemaphoreType.DMA((16,)),
                pltpu.SemaphoreType.DMA((2,)),
            ],
            compiler_params=pltpu.CompilerParams(vmem_limit_bytes=VMEM_LIMIT),
        )(v_cache, z_cache, long_filt)

        dma = pltpu.SemaphoreType.DMA
        chunk = (rows, chan)
        fin, vzp = pl.pallas_call(
            dense_kernel,
            name="dense_kernel",
            out_shape=(sds((sp_size, 4) + chunk, F32), sds((sp_size, NUM_LAYERS, 56, chan), F32)),
            in_specs=[vmem] * 6 + [hbm] * 8,
            out_specs=(hbm, hbm),
            scratch_shapes=[
                pltpu.VMEM((2, 3, dim, chan), BF16),
                pltpu.VMEM((2, chan, dim), BF16),
                pltpu.VMEM((2, dim, w_up.shape[-1]), BF16),
                pltpu.VMEM((2, w_down.shape[1], dim), BF16),
                pltpu.VMEM((2, 2, 8, chan), F32),
                pltpu.VMEM((3, rows + 8, chan), F32),
                pltpu.VMEM((2 * rows, chan), F32),
                pltpu.VMEM((rows, dim), BF16),
                pltpu.VMEM((rows, w_up.shape[-1]), BF16),
                pltpu.VMEM((4,) + chunk, F32),
                pltpu.VMEM((4, own, shard_len, chan), BF16),
                pltpu.VMEM((2, shard_len + 8, chan), F32),
                pltpu.VMEM((NUM_STEPS, shard_len, chan), F32),
                pltpu.VMEM((4, 4) + chunk, F32),
                pltpu.VMEM((4, 3) + chunk, F32),
                pltpu.VMEM((4, 3) + chunk, F32),
                pltpu.VMEM((4, 3) + chunk, F32),
                pltpu.VMEM((3, 4) + chunk, F32),
                pltpu.VMEM((4, 4) + chunk, F32),
                pltpu.VMEM((4, 2, 56, chan), F32),
                dma((2, 3)), dma(()), dma((2, 2)), dma((2, 4)), dma((2, 4)), dma(()), dma((8,)), dma((2,)),
                dma((4, 3)), dma((4, 3)), dma((4, 3)), dma((4, 3)), dma((4, 3)), dma((4, 3)), dma((4, 3)), dma((4, 3)),
                dma((2, 3)), dma((2, 3)),
            ],
            compiler_params=pltpu.CompilerParams(collective_id=0, has_side_effects=True, vmem_limit_bytes=VMEM_LIMIT),
        )(step_emb, jnp.transpose(short_state, (0, 1, 3, 2, 4)), jnp.transpose(b_in, (1, 0, 2)), jnp.transpose(short_taps, (1, 2, 0, 3)),
          skip_gain, b_out, part, v_cache, z_cache, long_filt, jnp.transpose(w_in, (0, 2, 1, 3)), w_out, w_up, w_down)

        hidden, states, v_out, z_out = pl.pallas_call(
            finish_kernel,
            name="finish_kernel",
            out_shape=(sds((NUM_STEPS, num_seq, dim), F32), sds((NUM_LAYERS, num_seq, 3, 2, chan), BF16),
                       sds(v_cache.shape, BF16), sds(z_cache.shape, BF16)),
            in_specs=[vmem, vmem, hbm, hbm],
            out_specs=(vmem, vmem, hbm, hbm),
            input_output_aliases={2: 2, 3: 3},
            scratch_shapes=[pltpu.VMEM((2, NUM_LAYERS, num_seq, 8, chan), BF16), dma((2,))],
            compiler_params=pltpu.CompilerParams(vmem_limit_bytes=VMEM_LIMIT),
        )(fin, vzp, v_out, z_out)
        return (hidden, v_out, z_out, jnp.transpose(states, (0, 1, 3, 2, 4)))

    specs_in = (
        P(None, "dp", None),
        P(None, "dp", "sp", "tp"),
        P(None, "dp", "sp", "tp"),
        P(None, "dp", None, None, "tp"),
        P(None, None, None, "tp"),
        P(None, None, "tp"),
        P(None, None, None, "tp"),
        P(None, None, None, "tp"),
        P(None, None, "tp"),
        P(None, "tp", None),
        P(None, None),
        P(None, None, "tp"),
        P(None, "tp", None),
    )
    specs_out = (
        P(None, "dp", None),
        P(None, "dp", "sp", "tp"),
        P(None, "dp", "sp", "tp"),
        P(None, "dp", None, None, "tp"),
    )
    return jax.shard_map(device_fn, mesh=mesh, in_specs=specs_in, out_specs=specs_out, check_vma=False)
```

```python
import jax
import jax.numpy as jnp
from jax import lax
from jax.experimental import pallas as pl
from jax.experimental.pallas import tpu as pltpu
from jax.sharding import PartitionSpec as P

NUM_STEPS = 4
NUM_LAYERS = 2
MESH = pl.DeviceIdType.MESH
F32 = jnp.float32
BF16 = jnp.bfloat16
VMEM_LIMIT = 66_500_000
AHEAD = 8
SUB = 1


def shift_filters(fwin, fsh):
    groups = fsh.shape[1] // 8
    sub = lax.broadcasted_iota(jnp.int32, (8, fsh.shape[2]), 0)

    def prep(g, prev):
        cur = fwin[pl.ds(pl.multiple_of((groups - 1 - g) * 8, 8), 8), :]
        for j in range(NUM_STEPS):
            mixed = jnp.where(sub <= j, prev, cur)
            fsh[j, pl.ds(pl.multiple_of(g * 8, 8), 8), :] = jnp.take_along_axis(mixed, (j - sub) % 8, axis=0)
        return cur

    lax.fori_loop(0, groups, prep, fwin[pl.ds(groups * 8, 8), :])


def conv_unit(buf, fsh, out):
    own, shard_len, chan = buf.shape

    def block_body(i, carry):
        lanes = pl.ds(pl.multiple_of(i * 128, 128), 128)
        accs = [jnp.zeros((8, 128), F32)] * (own * NUM_STEPS)
        for g in range(shard_len // 16):
            rows = pl.ds(g * 16, 16)
            filts = [fsh[j, rows, lanes] for j in range(NUM_STEPS)]
            for b in range(own):
                v = buf[b, rows, lanes].astype(F32)
                for j in range(NUM_STEPS):
                    m = v * filts[j]
                    accs[j * own + b] = accs[j * own + b] + m[:8] + m[8:]
        for row in range(own * NUM_STEPS):
            out[row:row + 1, lanes] = jnp.sum(accs[row], axis=0, keepdims=True)
        return carry

    lax.fori_loop(0, chan // 128, block_body, 0)


def window_base(shard_len):
    return pl.multiple_of(jnp.maximum((2 - lax.axis_index("sp")) * shard_len, 0), 8)


def conv_kernel(v_ref, z_ref, f_ref, vo_ref, zo_ref, part_out, buf, fwin, fsh, part_ref, rsem, wsem, fsem, psem):
    shard_len = v_ref.shape[2]
    base = window_base(shard_len)
    filt_copies = [pltpu.make_async_copy(f_ref.at[0, a, pl.ds(base, shard_len + 8)], fwin.at[a], fsem.at[a]) for a in range(2)]
    order = []
    for i in range(8):
        order += [(0, i // 4, i % 4), (1, i // 4, i % 4)]
    reads = [pltpu.make_async_copy((v_ref, z_ref)[a].at[layer, pl.ds(4 * q, 4)], buf.at[n], rsem.at[n])
             for n, (layer, a, q) in enumerate(order)]
    writes = [pltpu.make_async_copy(buf.at[n], (vo_ref, zo_ref)[a].at[layer, pl.ds(4 * q, 4)], wsem.at[n])
              for n, (layer, a, q) in enumerate(order)]
    part_copies = [pltpu.make_async_copy(part_ref.at[a], part_out.at[a], psem.at[a]) for a in range(2)]
    filt_copies[0].start()
    for n in range(AHEAD):
        reads[n].start()
    filt_copies[1].start()
    done = 0

    def pass_on(upto):
        for n in range(done, upto):
            reads[n].wait()
            writes[n].start()
            if n + AHEAD < 16:
                reads[n + AHEAD].start()

    for i in range(8):
        a, q = divmod(i, 4)
        pass_on(min(2 * i + 3, 16))
        done = min(2 * i + 3, 16)
        if q == 0:
            filt_copies[a].wait()
            shift_filters(fwin.at[a], fsh)
        conv_unit(buf.at[2 * i], fsh, part_ref.at[a, q])
        if q == 3:
            part_copies[a].start()
    for copy in writes + part_copies:
        copy.wait()


def dense_kernel(emb_hbm, state_hbm, b_in_hbm, taps_hbm, skip_hbm, b_out_hbm, part_hbm, v_ref, z_ref, f_ref, w_in_ref, w_out_ref, w_up_ref, w_down_ref,
                 hid_out, state_out, rows_out,
                 emb_ref, state_ref, b_in_ref, taps_ref, skip_ref, b_out_ref,
                 w_in, w_out, w_up, w_down, lags, ext, shifted, xrow, inner, emb,
                 buf, fwin, fsh, part_ref, part_in, rs_out, rs_in, hid, fin, vzp, hid_v, state_v, rows_v,
                 in_sem, lag_sem, out_sem, up_sem, down_sem, own_sem, buf_sem, fwin_sem, fin_sem, small_sem,
                 part_send, part_recv, rs_send, rs_recv, ag_send, ag_recv, fin_send, fin_recv, vzp_send, vzp_recv):
    t = lax.axis_index("tp")
    s = lax.axis_index("sp")
    flip_t = (3 - t, (t + 2) % 4, t + 1 - 2 * (t % 2))
    flip_s = (3 - s, (s + 2) % 4, s + 1 - 2 * (s % 2))
    middle = (t + 1) // 2 % 2
    slot_t = (middle, 1 - middle, 2)
    peer_t = (flip_t[0] + middle * (flip_t[1] - flip_t[0]), flip_t[1] + middle * (flip_t[0] - flip_t[1]), flip_t[2])
    rows = NUM_STEPS * 4
    cols = ext.shape[-1]
    dim = 4 * cols
    width = cols // SUB

    in_copies = [[pltpu.make_async_copy(w_in_ref.at[l, g], w_in.at[l, g], in_sem.at[l, g]) for g in range(3)] for l in range(2)]
    out_copies = [[pltpu.make_async_copy(w_out_ref.at[l, pl.ds(256 * i, 256)], w_out.at[l, pl.ds(256 * i, 256)], out_sem.at[l, i])
                   for i in range(cols // 256)] for l in range(2)]
    up_copies = [[pltpu.make_async_copy(w_up_ref.at[l, pl.ds(512 * i, 512)], w_up.at[l, pl.ds(512 * i, 512)], up_sem.at[l, i])
                  for i in range(4)] for l in range(2)]
    down_copies = [[pltpu.make_async_copy(w_down_ref.at[l, pl.ds(512 * i, 512)], w_down.at[l, pl.ds(512 * i, 512)], down_sem.at[l, i])
                    for i in range(4)] for l in range(2)]
    lag_copy = pltpu.make_async_copy(f_ref.at[:, :, pl.ds(0, 8)], lags, lag_sem)

    def start(copies):
        for copy in copies:
            copy.start()

    def wait(copies):
        for copy in copies:
            copy.wait()

    part_copy = pltpu.make_async_copy(part_hbm, part_ref.at[pl.ds(0, 2)], own_sem)
    shard_len = v_ref.shape[2]
    fwin_copies = [pltpu.make_async_copy(f_ref.at[1, a, pl.ds(window_base(shard_len), shard_len + 8)], fwin.at[a], fwin_sem.at[a])
                   for a in range(2)]
    reads = [pltpu.make_async_copy((v_ref, z_ref)[n // 4].at[1, pl.ds(4 * (n % 4), 4)], buf.at[n % 4], buf_sem.at[n]) for n in range(8)]
    small_copies = [pltpu.make_async_copy(src, dst, small_sem.at[i]) for i, (src, dst) in enumerate((
        (emb_hbm, emb_ref), (state_hbm, state_ref), (b_in_hbm, b_in_ref), (taps_hbm, taps_ref), (skip_hbm, skip_ref), (b_out_hbm, b_out_ref)))]
    start(small_copies)
    part_copy.start()
    start(in_copies[0])
    lag_copy.start()
    start(out_copies[0])

    barrier = pltpu.get_barrier_semaphore()
    for k in range(3):
        pl.semaphore_signal(barrier, inc=1, device_id={"tp": flip_t[k]}, device_id_type=MESH)
        pl.semaphore_signal(barrier, inc=1, device_id={"sp": flip_s[k]}, device_id_type=MESH)
    pl.semaphore_wait(barrier, 6)

    wait(small_copies)
    for k in range(4):
        @pl.when(s == k)
        def _():
            for j in range(NUM_STEPS):
                for i in range(4):
                    for u in range(SUB):
                        first = cols * i + width * u
                        emb[i, u, 4 * j:4 * j + 4] = emb_ref[j, :, first:first + width].astype(F32)[4 * k:4 * k + 4]

    sends = []

    def send(src, dst, send_sem, recv_sem, device_id):
        copy = pltpu.make_async_remote_copy(src_ref=src, dst_ref=dst, send_sem=send_sem, recv_sem=recv_sem,
                                            device_id=device_id, device_id_type=MESH)
        copy.start()
        sends.append(copy)
        return copy

    part_copy.wait()
    def send_part(a):
        return [send(part_ref.at[a, flip_s[k]], part_in.at[a, k], part_send.at[a, k], part_recv.at[a, k], {"sp": flip_s[k]})
                for k in range(3)]

    part_copies = [send_part(0), send_part(1), None, None]

    def cached_terms(a, first, count):
        if first == 0:
            fwin_copies[a].wait()
            shift_filters(fwin.at[a], fsh)
        for q in range(first, first + count):
            n = 4 * a + q
            reads[n].wait()
            conv_unit(buf.at[q], fsh, part_ref.at[2 + a, q])
            if n + 4 < 8:
                reads[n + 4].start()
        if first + count == 4:
            part_copies[2 + a] = send_part(2 + a)

    def order_rows(l):
        for copy in vzp_copies[l]:
            copy.wait_recv()
        for g in range(4):
            for c in range(3):
                for b in range(4):
                    first = 8 * c + b
                    pair = jnp.concatenate([vzp[g, l, first:first + 1], vzp[g, l, first + 4:first + 5]], axis=0)
                    state_v[l, 4 * g + b, c] = pair.astype(BF16)

        @pl.when(s == 3)
        def _():
            for a in range(2):
                for g in range(4):
                    for b in range(4):
                        first = 24 + 16 * a + b
                        new = [vzp[g, l, first + 4 * j:first + 4 * j + 1] for j in range(NUM_STEPS)]
                        new = jnp.concatenate(new + [jnp.zeros((4, cols), F32)], axis=0)
                        rows_v[a, l, 4 * g + b] = new.astype(BF16)

    def norm_to_xrow(pieces):
        mean = sum(jnp.sum(c, axis=-1, keepdims=True) for c in pieces) / dim
        cent = [c - mean for c in pieces]
        var = sum(jnp.sum(c * c, axis=-1, keepdims=True) for c in cent) / dim
        scale = lax.rsqrt(var + 1e-5)
        for i, c in enumerate(cent):
            xrow[:, width * i:width * (i + 1)] = (c * scale).astype(BF16)

    def reduce_gather(r, act, weight, base_ref, bias_of, out_ref):
        def piece(c, u):
            return jnp.dot(act, weight[:, pl.ds(pl.multiple_of(c * cols + u * width, width), width)], preferred_element_type=F32)

        copies = []
        for u in range(SUB):
            for k, peer in zip(slot_t, peer_t):
                rs_out[r, k, u] = piece(peer, u)
                copies.append(send(rs_out.at[r, k, u], rs_in.at[r, k, u], rs_send.at[r, k, u], rs_recv.at[r, k, u], {"tp": peer}))
        totals = [base_ref[t, u] + piece(t, u) for u in range(SUB)]
        if bias_of is not None:
            totals = [total + bias_of(u) for u, total in enumerate(totals)]
        if r == 0:
            cached_terms(0, 0, 3)
        if r == 1:
            cached_terms(1, 1, 3)
        if r == 2:
            order_rows(0)
        gathers = []
        for u in range(SUB):
            total = totals[u]
            for k in (2, 1, 0):
                copies[3 * u + k].wait_recv()
                total = total + rs_in[r, slot_t[k], u]
            out_ref[t, u] = total
            own = out_ref.at[t, u]
            gathers.append([send(own, own, ag_send.at[r, k, u], ag_recv.at[r, k, u], {"tp": peer}) for k, peer in zip(slot_t, peer_t)])
        if r == 0:
            cached_terms(0, 3, 1)
            cached_terms(1, 0, 1)
        return gathers

    def wait_gather(gathers):
        for copies in gathers:
            for copy in copies:
                copy.wait_recv()

    def pieces_of(ref):
        return [ref[i, u] for i in range(4) for u in range(SUB)]

    vzp_copies = []
    shifted[0:rows, :] = jnp.zeros((rows, cols), F32)
    for l in range(NUM_LAYERS):
        base = emb if l == 0 else hid.at[2 * l - 1]
        norm_to_xrow(pieces_of(base))
        x = xrow[...]
        for g in range(3):
            in_copies[l][g].wait()
            proj = jnp.dot(x, w_in[l, g], preferred_element_type=F32) + b_in_ref[g, l:l + 1]
            proj = proj.astype(BF16).astype(F32)
            ext[g, 8:24] = proj
            for b in range(4):
                old = state_ref[l, 4 * s + b, g].astype(F32)
                ext[g, b:b + 1] = old[0:1]
                ext[g, 4 + b:5 + b] = old[1:2]
            vzp[s, l, 8 * g:8 * g + 8] = proj[8:16]
        if l == 0:
            start(fwin_copies)
            start(reads[:4])
        start(up_copies[l])
        start(down_copies[l])

        def mixed(g):
            return (taps_ref[0, g, l:l + 1] * ext[g, 8:24] + taps_ref[1, g, l:l + 1] * ext[g, 4:20]
                    + taps_ref[2, g, l:l + 1] * ext[g, 0:16])

        def conv(which, new):
            a = 2 * l + which
            if a == 0:
                lag_copy.wait()
            shifted[rows:2 * rows, :] = new
            acc = skip_ref[l, which:which + 1] * new
            for d in range(NUM_STEPS):
                acc = acc + lags[l, which, d:d + 1] * shifted[rows - 4 * d:2 * rows - 4 * d]
            acc = acc + part_ref[a, s]
            for k in range(3):
                part_copies[a][k].wait_recv()
                acc = acc + part_in[a, k]
            return acc

        v_new = mixed(2).astype(BF16).astype(F32)
        vzp[s, l, 24:40] = v_new
        z_new = (mixed(0) * conv(0, v_new)).astype(BF16).astype(F32)
        vzp[s, l, 40:56] = z_new
        y = (mixed(1) * conv(1, z_new)).astype(BF16)
        wait(out_copies[l])
        bias = [b_out_ref[l:l + 1, pl.ds(pl.multiple_of(t * cols + u * width, width), width)] for u in range(SUB)]
        gathers = reduce_gather(2 * l, y, w_out.at[l], base, lambda u: bias[u], hid.at[2 * l])
        vzp_copies.append([send(vzp.at[s, l], vzp.at[s, l], vzp_send.at[l, k], vzp_recv.at[l, k], {"sp": flip_s[k]}) for k in range(3)])
        if l == 0:
            start(in_copies[1])
            start(out_copies[1])
        wait_gather(gathers)
        norm_to_xrow(pieces_of(hid.at[2 * l]))
        x = xrow[...]
        wait(up_copies[l])
        for i in range(4):
            up = jnp.dot(x, w_up[l, :, cols * i:cols * (i + 1)], preferred_element_type=F32)
            inner[:, cols * i:cols * (i + 1)] = jax.nn.gelu(up).astype(BF16)
        act = inner[...]
        wait(down_copies[l])
        if l == 0:
            wait_gather(reduce_gather(1, act, w_down.at[l], hid.at[0], None, hid.at[1]))
        else:
            gathers = reduce_gather(3, act, w_down.at[l], hid.at[2], None, fin.at[s])

    def place(g, i, u):
        first = pl.multiple_of(cols * i + width * u, width)
        for k in range(4):
            @pl.when(g == k)
            def _():
                for j in range(NUM_STEPS):
                    hid_v[j, 4 * k:4 * k + 4, pl.ds(first, width)] = fin[k, i, u, 4 * j:4 * j + 4]

    chunk_ids = (t,) + peer_t
    order = [(i, u) for u in range(SUB) for i in (0, 3, 2, 1)]
    fin_copies = []
    for i, u in order:
        if i == 3 and u == 0:
            order_rows(1)
            pltpu.make_async_copy(state_v, state_out, fin_sem.at[1]).start()

            @pl.when(s == 3)
            def _():
                pltpu.make_async_copy(rows_v, rows_out, fin_sem.at[2]).start()

        if i > 0:
            gathers[u][i - 1].wait_recv()
        chunk = fin.at[s, chunk_ids[i], u]
        fin_copies.append([send(chunk, chunk, fin_send.at[i, k, u], fin_recv.at[i, k, u], {"sp": flip_s[k]}) for k in (2, 1, 0)])
        place(s, chunk_ids[i], u)
    for n, (i, u) in enumerate(order):
        for k in range(3):
            fin_copies[n][k].wait_recv()
            place(flip_s[2 - k], chunk_ids[i], u)
    hid_copy = pltpu.make_async_copy(hid_v, hid_out, fin_sem.at[0])
    hid_copy.start()
    pltpu.make_async_copy(state_v, state_out, fin_sem.at[1]).wait()

    @pl.when(s == 3)
    def _():
        pltpu.make_async_copy(rows_v, rows_out, fin_sem.at[2]).wait()

    hid_copy.wait()
    for copy in sends:
        copy.wait_send()


def finish_kernel(hid_ref, state_ref, rows_ref, v_ref, z_ref, hid_out, state_out, vo_ref, zo_ref, hid, state, rows, in_sem, out_sem):
    last = lax.axis_index("sp") == 3
    hid_in = [pltpu.make_async_copy(hid_ref.at[j], hid.at[j], in_sem.at[j]) for j in range(NUM_STEPS)]
    hid_put = [pltpu.make_async_copy(hid.at[j], hid_out.at[j], out_sem.at[j]) for j in range(NUM_STEPS)]
    state_in = pltpu.make_async_copy(state_ref, state, in_sem.at[4])
    state_put = pltpu.make_async_copy(state, state_out, out_sem.at[4])
    rows_in = [pltpu.make_async_copy(rows_ref.at[a], rows.at[a], in_sem.at[5 + a]) for a in range(2)]
    rows_put = [pltpu.make_async_copy(rows.at[a], dst.at[:, :, pl.ds(0, 8)], out_sem.at[5 + a]) for a, dst in enumerate((vo_ref, zo_ref))]

    @pl.when(last)
    def _():
        for copy in rows_in:
            copy.start()

    for copy in [state_in] + hid_in:
        copy.start()

    @pl.when(last)
    def _():
        for before, after in zip(rows_in, rows_put):
            before.wait()
            after.start()

    for before, after in zip([state_in] + hid_in, [state_put] + hid_put):
        before.wait()
        after.start()
    for copy in [state_put] + hid_put:
        copy.wait()

    @pl.when(last)
    def _():
        for copy in rows_put:
            copy.wait()


def solution(mesh):
    sp_size = mesh.shape["sp"]

    def device_fn(step_emb, v_cache, z_cache, short_state, w_in, b_in, short_taps, long_filt, skip_gain, w_out, b_out, w_up, w_down):
        num_seq, shard_len, chan = v_cache.shape[1:]
        dim = step_emb.shape[-1]
        own = num_seq // sp_size
        rows = NUM_STEPS * own
        hbm = pl.BlockSpec(memory_space=pl.ANY)
        sds = jax.ShapeDtypeStruct

        v_out, z_out, part = pl.pallas_call(
            conv_kernel,
            name="conv_kernel",
            out_shape=(sds(v_cache.shape, BF16), sds(z_cache.shape, BF16), sds((2, sp_size, rows, chan), F32)),
            in_specs=[hbm] * 3,
            out_specs=(hbm, hbm, hbm),
            scratch_shapes=[
                pltpu.VMEM((16, own, shard_len, chan), BF16),
                pltpu.VMEM((2, shard_len + 8, chan), F32),
                pltpu.VMEM((NUM_STEPS, shard_len, chan), F32),
                pltpu.VMEM((2, sp_size, rows, chan), F32),
                pltpu.SemaphoreType.DMA((16,)),
                pltpu.SemaphoreType.DMA((16,)),
                pltpu.SemaphoreType.DMA((2,)),
                pltpu.SemaphoreType.DMA((2,)),
            ],
            compiler_params=pltpu.CompilerParams(vmem_limit_bytes=VMEM_LIMIT),
        )(v_cache, z_cache, long_filt)

        dma = pltpu.SemaphoreType.DMA
        chunk = (SUB, rows, chan // SUB)
        state_shape = sds((NUM_LAYERS, num_seq, 3, 2, chan), BF16)
        hid_shape = sds((NUM_STEPS, num_seq, dim), F32)
        rows_shape = sds((2, NUM_LAYERS, num_seq, 8, chan), BF16)
        hidden, states, new_rows = pl.pallas_call(
            dense_kernel,
            name="dense_kernel",
            out_shape=(hid_shape, state_shape, rows_shape),
            in_specs=[hbm] * 14,
            out_specs=(hbm, hbm, hbm),
            scratch_shapes=[
                pltpu.VMEM(step_emb.shape, BF16),
                pltpu.VMEM(state_shape.shape, BF16),
                pltpu.VMEM((3, NUM_LAYERS, chan), F32),
                pltpu.VMEM((3, 3, NUM_LAYERS, chan), F32),
                pltpu.VMEM((NUM_LAYERS, 2, chan), F32),
                pltpu.VMEM((NUM_LAYERS, dim), F32),
                pltpu.VMEM((2, 3, dim, chan), BF16),
                pltpu.VMEM((2, chan, dim), BF16),
                pltpu.VMEM((2, dim, w_up.shape[-1]), BF16),
                pltpu.VMEM((2, w_down.shape[1], dim), BF16),
                pltpu.VMEM((2, 2, 8, chan), F32),
                pltpu.VMEM((3, rows + 8, chan), F32),
                pltpu.VMEM((2 * rows, chan), F32),
                pltpu.VMEM((rows, dim), BF16),
                pltpu.VMEM((rows, w_up.shape[-1]), BF16),
                pltpu.VMEM((4,) + chunk, F32),
                pltpu.VMEM((4, own, shard_len, chan), BF16),
                pltpu.VMEM((2, shard_len + 8, chan), F32),
                pltpu.VMEM((NUM_STEPS, shard_len, chan), F32),
                pltpu.VMEM((4, sp_size, rows, chan), F32),
                pltpu.VMEM((4, 3, rows, chan), F32),
                pltpu.VMEM((4, 3) + chunk, F32),
                pltpu.VMEM((4, 3) + chunk, F32),
                pltpu.VMEM((3, 4) + chunk, F32),
                pltpu.VMEM((4, 4) + chunk, F32),
                pltpu.VMEM((4, 2, 56, chan), F32),
                pltpu.VMEM(hid_shape.shape, F32),
                pltpu.VMEM(state_shape.shape, BF16),
                pltpu.VMEM(rows_shape.shape, BF16),
                dma((2, 3)), dma(()), dma((2, 2)), dma((2, 4)), dma((2, 4)), dma(()), dma((8,)), dma((2,)), dma((3,)), dma((6,)),
                dma((4, 3)), dma((4, 3)), dma((4, 3, SUB)), dma((4, 3, SUB)), dma((4, 3, SUB)), dma((4, 3, SUB)), dma((4, 3, SUB)), dma((4, 3, SUB)),
                dma((2, 3)), dma((2, 3)),
            ],
            compiler_params=pltpu.CompilerParams(collective_id=0, has_side_effects=True, vmem_limit_bytes=VMEM_LIMIT),
        )(step_emb, jnp.transpose(short_state, (0, 1, 3, 2, 4)), jnp.transpose(b_in, (1, 0, 2)), jnp.transpose(short_taps, (1, 2, 0, 3)),
          skip_gain, b_out, part, v_cache, z_cache, long_filt, jnp.transpose(w_in, (0, 2, 1, 3)), w_out, w_up, w_down)

        hidden, states, v_out, z_out = pl.pallas_call(
            finish_kernel,
            name="finish_kernel",
            out_shape=(hid_shape, state_shape, sds(v_cache.shape, BF16), sds(z_cache.shape, BF16)),
            in_specs=[hbm] * 5,
            out_specs=(hbm,) * 4,
            input_output_aliases={3: 2, 4: 3},
            scratch_shapes=[pltpu.VMEM(hid_shape.shape, F32), pltpu.VMEM(state_shape.shape, BF16), pltpu.VMEM(rows_shape.shape, BF16),
                            dma((7,)), dma((7,))],
            compiler_params=pltpu.CompilerParams(vmem_limit_bytes=VMEM_LIMIT),
        )(hidden, states, new_rows, v_out, z_out)
        return (hidden, v_out, z_out, jnp.transpose(states, (0, 1, 3, 2, 4)))

    specs_in = (
        P(None, "dp", None),
        P(None, "dp", "sp", "tp"),
        P(None, "dp", "sp", "tp"),
        P(None, "dp", None, None, "tp"),
        P(None, None, None, "tp"),
        P(None, None, "tp"),
        P(None, None, None, "tp"),
        P(None, None, None, "tp"),
        P(None, None, "tp"),
        P(None, "tp", None),
        P(None, None),
        P(None, None, "tp"),
        P(None, "tp", None),
    )
    specs_out = (
        P(None, "dp", None),
        P(None, "dp", "sp", "tp"),
        P(None, "dp", "sp", "tp"),
        P(None, "dp", None, None, "tp"),
    )
    return jax.shard_map(device_fn, mesh=mesh, in_specs=specs_in, out_specs=specs_out, check_vma=False)
```

```python
import jax
import jax.numpy as jnp
from jax import lax
from jax.experimental import pallas as pl
from jax.experimental.pallas import tpu as pltpu
from jax.sharding import PartitionSpec as P

NUM_STEPS = 4
NUM_LAYERS = 2
MESH = pl.DeviceIdType.MESH
F32 = jnp.float32
BF16 = jnp.bfloat16
VMEM_LIMIT = 66_500_000
AHEAD = 10
SUB = 1


def shift_filters(fwin, fsh):
    groups = fsh.shape[1] // 8
    sub = lax.broadcasted_iota(jnp.int32, (8, fsh.shape[2]), 0)

    def prep(g, prev):
        cur = fwin[pl.ds(pl.multiple_of((groups - 1 - g) * 8, 8), 8), :]
        for j in range(NUM_STEPS):
            mixed = jnp.where(sub <= j, prev, cur)
            fsh[j, pl.ds(pl.multiple_of(g * 8, 8), 8), :] = jnp.take_along_axis(mixed, (j - sub) % 8, axis=0)
        return cur

    lax.fori_loop(0, groups, prep, fwin[pl.ds(groups * 8, 8), :])


def conv_unit(buf, fsh, out):
    own, shard_len, chan = buf.shape

    def block_body(i, carry):
        lanes = pl.ds(pl.multiple_of(i * 128, 128), 128)
        accs = [jnp.zeros((8, 128), F32)] * (own * NUM_STEPS)
        for g in range(shard_len // 16):
            rows = pl.ds(g * 16, 16)
            filts = [fsh[j, rows, lanes] for j in range(NUM_STEPS)]
            for b in range(own):
                v = buf[b, rows, lanes].astype(F32)
                for j in range(NUM_STEPS):
                    m = v * filts[j]
                    accs[j * own + b] = accs[j * own + b] + m[:8] + m[8:]
        for row in range(own * NUM_STEPS):
            out[row:row + 1, lanes] = jnp.sum(accs[row], axis=0, keepdims=True)
        return carry

    lax.fori_loop(0, chan // 128, block_body, 0)


def window_base(shard_len):
    return pl.multiple_of(jnp.maximum((2 - lax.axis_index("sp")) * shard_len, 0), 8)


def conv_kernel(v_ref, z_ref, f_ref, vo_ref, zo_ref, part_out, buf, fwin, fsh, part_ref, rsem, wsem, fsem, psem):
    shard_len = v_ref.shape[2]
    base = window_base(shard_len)
    filt_copies = [pltpu.make_async_copy(f_ref.at[0, a, pl.ds(base, shard_len + 8)], fwin.at[a], fsem.at[a]) for a in range(2)]
    order = []
    for i in range(8):
        order += [(0, i // 4, i % 4), (1, i // 4, i % 4)]
    reads = [pltpu.make_async_copy((v_ref, z_ref)[a].at[layer, pl.ds(4 * q, 4)], buf.at[n], rsem.at[n])
             for n, (layer, a, q) in enumerate(order)]
    writes = [pltpu.make_async_copy(buf.at[n], (vo_ref, zo_ref)[a].at[layer, pl.ds(4 * q, 4)], wsem.at[n])
              for n, (layer, a, q) in enumerate(order)]
    part_copies = [pltpu.make_async_copy(part_ref.at[a], part_out.at[a], psem.at[a]) for a in range(2)]
    filt_copies[0].start()
    for n in range(AHEAD):
        reads[n].start()
    filt_copies[1].start()
    done = 0

    def pass_on(upto):
        for n in range(done, upto):
            reads[n].wait()
            writes[n].start()
            if n + AHEAD < 16:
                reads[n + AHEAD].start()

    for i in range(8):
        a, q = divmod(i, 4)
        pass_on(min(2 * i + 3, 16))
        done = min(2 * i + 3, 16)
        if q == 0:
            filt_copies[a].wait()
            shift_filters(fwin.at[a], fsh)
        conv_unit(buf.at[2 * i], fsh, part_ref.at[a, q])
        if q == 3:
            part_copies[a].start()
    for copy in writes + part_copies:
        copy.wait()


def dense_kernel(emb_hbm, state_hbm, b_in_hbm, taps_hbm, skip_hbm, b_out_hbm, part_hbm, v_ref, z_ref, f_ref, w_in_ref, w_out_ref, w_up_ref, w_down_ref,
                 hid_out, state_out, rows_out,
                 emb_ref, state_ref, b_in_ref, taps_ref, skip_ref, b_out_ref,
                 w_in, w_out, w_up, w_down, lags, ext, shifted, xrow, inner, emb,
                 buf, fwin, fsh, part_ref, part_in, rs_out, rs_in, hid, fin, vzp, hid_v, state_v, rows_v,
                 in_sem, lag_sem, out_sem, up_sem, down_sem, own_sem, buf_sem, fwin_sem, fin_sem, small_sem,
                 part_send, part_recv, rs_send, rs_recv, ag_send, ag_recv, fin_send, fin_recv, vzp_send, vzp_recv):
    t = lax.axis_index("tp")
    s = lax.axis_index("sp")
    flip_t = (3 - t, (t + 2) % 4, t + 1 - 2 * (t % 2))
    flip_s = (3 - s, (s + 2) % 4, s + 1 - 2 * (s % 2))
    middle = (t + 1) // 2 % 2
    slot_t = (middle, 1 - middle, 2)
    peer_t = (flip_t[0] + middle * (flip_t[1] - flip_t[0]), flip_t[1] + middle * (flip_t[0] - flip_t[1]), flip_t[2])
    rows = NUM_STEPS * 4
    cols = ext.shape[-1]
    dim = 4 * cols
    width = cols // SUB

    in_copies = [[pltpu.make_async_copy(w_in_ref.at[l, g], w_in.at[l, g], in_sem.at[l, g]) for g in range(3)] for l in range(2)]
    out_copies = [[pltpu.make_async_copy(w_out_ref.at[l, pl.ds(256 * i, 256)], w_out.at[l, pl.ds(256 * i, 256)], out_sem.at[l, i])
                   for i in range(cols // 256)] for l in range(2)]
    up_copies = [[pltpu.make_async_copy(w_up_ref.at[l, pl.ds(512 * i, 512)], w_up.at[l, pl.ds(512 * i, 512)], up_sem.at[l, i])
                  for i in range(4)] for l in range(2)]
    down_copies = [[pltpu.make_async_copy(w_down_ref.at[l, pl.ds(512 * i, 512)], w_down.at[l, pl.ds(512 * i, 512)], down_sem.at[l, i])
                    for i in range(4)] for l in range(2)]
    lag_copy = pltpu.make_async_copy(f_ref.at[:, :, pl.ds(0, 8)], lags, lag_sem)

    def start(copies):
        for copy in copies:
            copy.start()

    def wait(copies):
        for copy in copies:
            copy.wait()

    part_loads = [pltpu.make_async_copy(part_hbm.at[a], part_ref.at[a], own_sem.at[a]) for a in range(2)]
    shard_len = v_ref.shape[2]
    fwin_copies = [pltpu.make_async_copy(f_ref.at[1, a, pl.ds(window_base(shard_len), shard_len + 8)], fwin.at[a], fwin_sem.at[a])
                   for a in range(2)]
    reads = [pltpu.make_async_copy((v_ref, z_ref)[n // 4].at[1, pl.ds(4 * (n % 4), 4)], buf.at[n % 4], buf_sem.at[n]) for n in range(8)]
    small_copies = [pltpu.make_async_copy(src, dst, small_sem.at[i]) for i, (src, dst) in enumerate((
        (emb_hbm, emb_ref), (state_hbm, state_ref), (b_in_hbm, b_in_ref), (taps_hbm, taps_ref), (skip_hbm, skip_ref), (b_out_hbm, b_out_ref)))]
    start(part_loads)
    start(small_copies)
    start(in_copies[0])
    lag_copy.start()
    start(out_copies[0])

    barrier = pltpu.get_barrier_semaphore()
    for k in range(3):
        pl.semaphore_signal(barrier, inc=1, device_id={"tp": flip_t[k]}, device_id_type=MESH)
        pl.semaphore_signal(barrier, inc=1, device_id={"sp": flip_s[k]}, device_id_type=MESH)
    wait(small_copies)
    for k in range(4):
        @pl.when(s == k)
        def _():
            for j in range(NUM_STEPS):
                for i in range(4):
                    for u in range(SUB):
                        first = cols * i + width * u
                        emb[i, u, 4 * j:4 * j + 4] = emb_ref[j, :, first:first + width].astype(F32)[4 * k:4 * k + 4]
    pl.semaphore_wait(barrier, 6)

    sends = []

    def send(src, dst, send_sem, recv_sem, device_id):
        copy = pltpu.make_async_remote_copy(src_ref=src, dst_ref=dst, send_sem=send_sem, recv_sem=recv_sem,
                                            device_id=device_id, device_id_type=MESH)
        copy.start()
        sends.append(copy)
        return copy

    def send_part(a):
        if a < 2:
            part_loads[a].wait()
        return [send(part_ref.at[a, flip_s[k]], part_in.at[a, k], part_send.at[a, k], part_recv.at[a, k], {"sp": flip_s[k]})
                for k in range(3)]

    part_copies = [send_part(0), send_part(1), None, None]

    def cached_terms(a, first, count):
        if first == 0:
            fwin_copies[a].wait()
            shift_filters(fwin.at[a], fsh)
        for q in range(first, first + count):
            n = 4 * a + q
            reads[n].wait()
            conv_unit(buf.at[q], fsh, part_ref.at[2 + a, q])
            if n + 4 < 8:
                reads[n + 4].start()
        if first + count == 4:
            part_copies[2 + a] = send_part(2 + a)

    def order_rows(l):
        for copy in vzp_copies[l]:
            copy.wait_recv()
        for g in range(4):
            for c in range(3):
                for b in range(4):
                    first = 8 * c + b
                    pair = jnp.concatenate([vzp[g, l, first:first + 1], vzp[g, l, first + 4:first + 5]], axis=0)
                    state_v[l, 4 * g + b, c] = pair.astype(BF16)

        @pl.when(s == 3)
        def _():
            for a in range(2):
                for g in range(4):
                    for b in range(4):
                        first = 24 + 16 * a + b
                        new = [vzp[g, l, first + 4 * j:first + 4 * j + 1] for j in range(NUM_STEPS)]
                        new = jnp.concatenate(new + [jnp.zeros((4, cols), F32)], axis=0)
                        rows_v[a, l, 4 * g + b] = new.astype(BF16)

    def norm_to_xrow(pieces):
        mean = sum(jnp.sum(c, axis=-1, keepdims=True) for c in pieces) / dim
        cent = [c - mean for c in pieces]
        var = sum(jnp.sum(c * c, axis=-1, keepdims=True) for c in cent) / dim
        scale = lax.rsqrt(var + 1e-5)
        for i, c in enumerate(cent):
            xrow[:, width * i:width * (i + 1)] = (c * scale).astype(BF16)

    def reduce_gather(r, act, weight, base_ref, bias_of, out_ref):
        def piece(c, u):
            return jnp.dot(act, weight[:, pl.ds(pl.multiple_of(c * cols + u * width, width), width)], preferred_element_type=F32)

        copies = []
        for u in range(SUB):
            for k, peer in zip(slot_t, peer_t):
                rs_out[r, k, u] = piece(peer, u)
                copies.append(send(rs_out.at[r, k, u], rs_in.at[r, k, u], rs_send.at[r, k, u], rs_recv.at[r, k, u], {"tp": peer}))
        totals = [base_ref[t, u] + piece(t, u) for u in range(SUB)]
        if bias_of is not None:
            totals = [total + bias_of(u) for u, total in enumerate(totals)]
        if r == 0:
            cached_terms(0, 0, 3)
        if r == 1:
            cached_terms(1, 1, 3)
        if r == 2:
            order_rows(0)
        gathers = []
        for u in range(SUB):
            total = totals[u]
            for k in (2, 1, 0):
                copies[3 * u + k].wait_recv()
                total = total + rs_in[r, slot_t[k], u]
            out_ref[t, u] = total
            own = out_ref.at[t, u]
            gathers.append([send(own, own, ag_send.at[r, k, u], ag_recv.at[r, k, u], {"tp": peer}) for k, peer in zip(slot_t, peer_t)])
        if r == 0:
            cached_terms(0, 3, 1)
            cached_terms(1, 0, 1)
        return gathers

    def wait_gather(gathers):
        for copies in gathers:
            for copy in copies:
                copy.wait_recv()

    def pieces_of(ref):
        return [ref[i, u] for i in range(4) for u in range(SUB)]

    vzp_copies = []
    shifted[0:rows, :] = jnp.zeros((rows, cols), F32)
    for l in range(NUM_LAYERS):
        base = emb if l == 0 else hid.at[2 * l - 1]
        norm_to_xrow(pieces_of(base))
        x = xrow[...]
        for g in range(3):
            in_copies[l][g].wait()
            proj = jnp.dot(x, w_in[l, g], preferred_element_type=F32) + b_in_ref[g, l:l + 1]
            proj = proj.astype(BF16).astype(F32)
            ext[g, 8:24] = proj
            for b in range(4):
                old = state_ref[l, 4 * s + b, g].astype(F32)
                ext[g, b:b + 1] = old[0:1]
                ext[g, 4 + b:5 + b] = old[1:2]
            vzp[s, l, 8 * g:8 * g + 8] = proj[8:16]
        if l == 0:
            start(fwin_copies)
            start(reads[:4])
        start(up_copies[l])
        start(down_copies[l])

        def mixed(g):
            return (taps_ref[0, g, l:l + 1] * ext[g, 8:24] + taps_ref[1, g, l:l + 1] * ext[g, 4:20]
                    + taps_ref[2, g, l:l + 1] * ext[g, 0:16])

        def conv(which, new):
            a = 2 * l + which
            if a == 0:
                lag_copy.wait()
            shifted[rows:2 * rows, :] = new
            acc = skip_ref[l, which:which + 1] * new
            for d in range(NUM_STEPS):
                acc = acc + lags[l, which, d:d + 1] * shifted[rows - 4 * d:2 * rows - 4 * d]
            acc = acc + part_ref[a, s]
            for k in range(3):
                part_copies[a][k].wait_recv()
                acc = acc + part_in[a, k]
            return acc

        v_new = mixed(2).astype(BF16).astype(F32)
        vzp[s, l, 24:40] = v_new
        z_new = (mixed(0) * conv(0, v_new)).astype(BF16).astype(F32)
        vzp[s, l, 40:56] = z_new
        y = (mixed(1) * conv(1, z_new)).astype(BF16)
        wait(out_copies[l])
        bias = [b_out_ref[l:l + 1, pl.ds(pl.multiple_of(t * cols + u * width, width), width)] for u in range(SUB)]
        gathers = reduce_gather(2 * l, y, w_out.at[l], base, lambda u: bias[u], hid.at[2 * l])
        vzp_copies.append([send(vzp.at[s, l], vzp.at[s, l], vzp_send.at[l, k], vzp_recv.at[l, k], {"sp": flip_s[k]}) for k in range(3)])
        if l == 0:
            start(in_copies[1])
            start(out_copies[1])
        wait_gather(gathers)
        norm_to_xrow(pieces_of(hid.at[2 * l]))
        x = xrow[...]
        wait(up_copies[l])
        for i in range(4):
            up = jnp.dot(x, w_up[l, :, cols * i:cols * (i + 1)], preferred_element_type=F32)
            inner[:, cols * i:cols * (i + 1)] = jax.nn.gelu(up).astype(BF16)
        act = inner[...]
        wait(down_copies[l])
        if l == 0:
            wait_gather(reduce_gather(1, act, w_down.at[l], hid.at[0], None, hid.at[1]))
        else:
            gathers = reduce_gather(3, act, w_down.at[l], hid.at[2], None, fin.at[s])

    def place(g, i, u):
        first = pl.multiple_of(cols * i + width * u, width)
        for k in range(4):
            @pl.when(g == k)
            def _():
                for j in range(NUM_STEPS):
                    hid_v[j, 4 * k:4 * k + 4, pl.ds(first, width)] = fin[k, i, u, 4 * j:4 * j + 4]

    chunk_ids = (t,) + peer_t
    order = [(i, u) for u in range(SUB) for i in (0, 3, 2, 1)]
    fin_copies = []
    for i, u in order:
        if i == 3 and u == 0:
            order_rows(1)
            pltpu.make_async_copy(state_v, state_out, fin_sem.at[1]).start()

            @pl.when(s == 3)
            def _():
                pltpu.make_async_copy(rows_v, rows_out, fin_sem.at[2]).start()

        if i > 0:
            gathers[u][i - 1].wait_recv()
        chunk = fin.at[s, chunk_ids[i], u]
        fin_copies.append([send(chunk, chunk, fin_send.at[i, k, u], fin_recv.at[i, k, u], {"sp": flip_s[k]}) for k in (2, 1, 0)])
        place(s, chunk_ids[i], u)
    for n, (i, u) in enumerate(order):
        for k in range(3):
            fin_copies[n][k].wait_recv()
            place(flip_s[2 - k], chunk_ids[i], u)
    hid_copy = pltpu.make_async_copy(hid_v, hid_out, fin_sem.at[0])
    hid_copy.start()
    pltpu.make_async_copy(state_v, state_out, fin_sem.at[1]).wait()

    @pl.when(s == 3)
    def _():
        pltpu.make_async_copy(rows_v, rows_out, fin_sem.at[2]).wait()

    hid_copy.wait()
    for copy in sends:
        copy.wait_send()


def finish_kernel(hid_ref, state_ref, rows_ref, v_ref, z_ref, hid_out, state_out, vo_ref, zo_ref, hid, state, rows, in_sem, out_sem):
    last = lax.axis_index("sp") == 3
    hid_in = [pltpu.make_async_copy(hid_ref.at[j], hid.at[j], in_sem.at[j]) for j in range(NUM_STEPS)]
    hid_put = [pltpu.make_async_copy(hid.at[j], hid_out.at[j], out_sem.at[j]) for j in range(NUM_STEPS)]
    state_in = pltpu.make_async_copy(state_ref, state, in_sem.at[4])
    state_put = pltpu.make_async_copy(state, state_out, out_sem.at[4])
    rows_in = [pltpu.make_async_copy(rows_ref.at[a], rows.at[a], in_sem.at[5 + a]) for a in range(2)]
    rows_put = [pltpu.make_async_copy(rows.at[a], dst.at[:, :, pl.ds(0, 8)], out_sem.at[5 + a]) for a, dst in enumerate((vo_ref, zo_ref))]

    @pl.when(last)
    def _():
        for copy in rows_in:
            copy.start()

    for copy in [state_in] + hid_in:
        copy.start()

    @pl.when(last)
    def _():
        for before, after in zip(rows_in, rows_put):
            before.wait()
            after.start()

    for before, after in zip([state_in] + hid_in, [state_put] + hid_put):
        before.wait()
        after.start()
    for copy in [state_put] + hid_put:
        copy.wait()

    @pl.when(last)
    def _():
        for copy in rows_put:
            copy.wait()


def solution(mesh):
    sp_size = mesh.shape["sp"]

    def device_fn(step_emb, v_cache, z_cache, short_state, w_in, b_in, short_taps, long_filt, skip_gain, w_out, b_out, w_up, w_down):
        num_seq, shard_len, chan = v_cache.shape[1:]
        dim = step_emb.shape[-1]
        own = num_seq // sp_size
        rows = NUM_STEPS * own
        hbm = pl.BlockSpec(memory_space=pl.ANY)
        sds = jax.ShapeDtypeStruct

        v_out, z_out, part = pl.pallas_call(
            conv_kernel,
            name="conv_kernel",
            out_shape=(sds(v_cache.shape, BF16), sds(z_cache.shape, BF16), sds((2, sp_size, rows, chan), F32)),
            in_specs=[hbm] * 3,
            out_specs=(hbm, hbm, hbm),
            scratch_shapes=[
                pltpu.VMEM((16, own, shard_len, chan), BF16),
                pltpu.VMEM((2, shard_len + 8, chan), F32),
                pltpu.VMEM((NUM_STEPS, shard_len, chan), F32),
                pltpu.VMEM((2, sp_size, rows, chan), F32),
                pltpu.SemaphoreType.DMA((16,)),
                pltpu.SemaphoreType.DMA((16,)),
                pltpu.SemaphoreType.DMA((2,)),
                pltpu.SemaphoreType.DMA((2,)),
            ],
            compiler_params=pltpu.CompilerParams(vmem_limit_bytes=VMEM_LIMIT),
        )(v_cache, z_cache, long_filt)

        dma = pltpu.SemaphoreType.DMA
        chunk = (SUB, rows, chan // SUB)
        state_shape = sds((NUM_LAYERS, num_seq, 3, 2, chan), BF16)
        hid_shape = sds((NUM_STEPS, num_seq, dim), F32)
        rows_shape = sds((2, NUM_LAYERS, num_seq, 8, chan), BF16)
        hidden, states, new_rows = pl.pallas_call(
            dense_kernel,
            name="dense_kernel",
            out_shape=(hid_shape, state_shape, rows_shape),
            in_specs=[hbm] * 14,
            out_specs=(hbm, hbm, hbm),
            scratch_shapes=[
                pltpu.VMEM(step_emb.shape, BF16),
                pltpu.VMEM(state_shape.shape, BF16),
                pltpu.VMEM((3, NUM_LAYERS, chan), F32),
                pltpu.VMEM((3, 3, NUM_LAYERS, chan), F32),
                pltpu.VMEM((NUM_LAYERS, 2, chan), F32),
                pltpu.VMEM((NUM_LAYERS, dim), F32),
                pltpu.VMEM((2, 3, dim, chan), BF16),
                pltpu.VMEM((2, chan, dim), BF16),
                pltpu.VMEM((2, dim, w_up.shape[-1]), BF16),
                pltpu.VMEM((2, w_down.shape[1], dim), BF16),
                pltpu.VMEM((2, 2, 8, chan), F32),
                pltpu.VMEM((3, rows + 8, chan), F32),
                pltpu.VMEM((2 * rows, chan), F32),
                pltpu.VMEM((rows, dim), BF16),
                pltpu.VMEM((rows, w_up.shape[-1]), BF16),
                pltpu.VMEM((4,) + chunk, F32),
                pltpu.VMEM((4, own, shard_len, chan), BF16),
                pltpu.VMEM((2, shard_len + 8, chan), F32),
                pltpu.VMEM((NUM_STEPS, shard_len, chan), F32),
                pltpu.VMEM((4, sp_size, rows, chan), F32),
                pltpu.VMEM((4, 3, rows, chan), F32),
                pltpu.VMEM((4, 3) + chunk, F32),
                pltpu.VMEM((4, 3) + chunk, F32),
                pltpu.VMEM((3, 4) + chunk, F32),
                pltpu.VMEM((4, 4) + chunk, F32),
                pltpu.VMEM((4, 2, 56, chan), F32),
                pltpu.VMEM(hid_shape.shape, F32),
                pltpu.VMEM(state_shape.shape, BF16),
                pltpu.VMEM(rows_shape.shape, BF16),
                dma((2, 3)), dma(()), dma((2, 2)), dma((2, 4)), dma((2, 4)), dma((2,)), dma((8,)), dma((2,)), dma((3,)), dma((6,)),
                dma((4, 3)), dma((4, 3)), dma((4, 3, SUB)), dma((4, 3, SUB)), dma((4, 3, SUB)), dma((4, 3, SUB)), dma((4, 3, SUB)), dma((4, 3, SUB)),
                dma((2, 3)), dma((2, 3)),
            ],
            compiler_params=pltpu.CompilerParams(collective_id=0, has_side_effects=True, vmem_limit_bytes=VMEM_LIMIT),
        )(step_emb, jnp.transpose(short_state, (0, 1, 3, 2, 4)), jnp.transpose(b_in, (1, 0, 2)), jnp.transpose(short_taps, (1, 2, 0, 3)),
          skip_gain, b_out, part, v_cache, z_cache, long_filt, jnp.transpose(w_in, (0, 2, 1, 3)), w_out, w_up, w_down)

        hidden, states, v_out, z_out = pl.pallas_call(
            finish_kernel,
            name="finish_kernel",
            out_shape=(hid_shape, state_shape, sds(v_cache.shape, BF16), sds(z_cache.shape, BF16)),
            in_specs=[hbm] * 5,
            out_specs=(hbm,) * 4,
            input_output_aliases={3: 2, 4: 3},
            scratch_shapes=[pltpu.VMEM(hid_shape.shape, F32), pltpu.VMEM(state_shape.shape, BF16), pltpu.VMEM(rows_shape.shape, BF16),
                            dma((7,)), dma((7,))],
            compiler_params=pltpu.CompilerParams(vmem_limit_bytes=VMEM_LIMIT),
        )(hidden, states, new_rows, v_out, z_out)
        return (hidden, v_out, z_out, jnp.transpose(states, (0, 1, 3, 2, 4)))

    specs_in = (
        P(None, "dp", None),
        P(None, "dp", "sp", "tp"),
        P(None, "dp", "sp", "tp"),
        P(None, "dp", None, None, "tp"),
        P(None, None, None, "tp"),
        P(None, None, "tp"),
        P(None, None, None, "tp"),
        P(None, None, None, "tp"),
        P(None, None, "tp"),
        P(None, "tp", None),
        P(None, None),
        P(None, None, "tp"),
        P(None, "tp", None),
    )
    specs_out = (
        P(None, "dp", None),
        P(None, "dp", "sp", "tp"),
        P(None, "dp", "sp", "tp"),
        P(None, "dp", None, None, "tp"),
    )
    return jax.shard_map(device_fn, mesh=mesh, in_specs=specs_in, out_specs=specs_out, check_vma=False)
```

```python
import jax
import jax.numpy as jnp
from jax import lax
from jax.experimental import pallas as pl
from jax.experimental.pallas import tpu as pltpu
from jax.sharding import PartitionSpec as P

NUM_STEPS = 4
NUM_LAYERS = 2
MESH = pl.DeviceIdType.MESH
F32 = jnp.float32
BF16 = jnp.bfloat16
VMEM_LIMIT = 66_500_000
AHEAD = 10
SUB = 1


def shift_filters(fwin, fsh):
    groups = fsh.shape[1] // 8
    sub = lax.broadcasted_iota(jnp.int32, (8, fsh.shape[2]), 0)

    def prep(g, prev):
        cur = fwin[pl.ds(pl.multiple_of((groups - 1 - g) * 8, 8), 8), :]
        for j in range(NUM_STEPS):
            mixed = jnp.where(sub <= j, prev, cur)
            fsh[j, pl.ds(pl.multiple_of(g * 8, 8), 8), :] = jnp.take_along_axis(mixed, (j - sub) % 8, axis=0)
        return cur

    lax.fori_loop(0, groups, prep, fwin[pl.ds(groups * 8, 8), :])


def conv_unit(buf, fsh, out):
    own, shard_len, chan = buf.shape

    def block_body(i, carry):
        lanes = pl.ds(pl.multiple_of(i * 128, 128), 128)
        accs = [jnp.zeros((8, 128), F32)] * (own * NUM_STEPS)
        for g in range(shard_len // 16):
            rows = pl.ds(g * 16, 16)
            filts = [fsh[j, rows, lanes] for j in range(NUM_STEPS)]
            for b in range(own):
                v = buf[b, rows, lanes].astype(F32)
                for j in range(NUM_STEPS):
                    m = v * filts[j]
                    accs[j * own + b] = accs[j * own + b] + m[:8] + m[8:]
        for row in range(own * NUM_STEPS):
            out[row:row + 1, lanes] = jnp.sum(accs[row], axis=0, keepdims=True)
        return carry

    lax.fori_loop(0, chan // 128, block_body, 0)


def window_base(shard_len):
    return pl.multiple_of(jnp.maximum((2 - lax.axis_index("sp")) * shard_len, 0), 8)


def conv_kernel(v_ref, z_ref, f_ref, vo_ref, zo_ref, part_out, buf, fwin, fsh, part_ref, rsem, wsem, fsem, psem):
    shard_len = v_ref.shape[2]
    base = window_base(shard_len)
    filt_copies = [pltpu.make_async_copy(f_ref.at[0, a, pl.ds(base, shard_len + 8)], fwin.at[a], fsem.at[a]) for a in range(2)]
    order = []
    for i in range(8):
        order += [(0, i // 4, i % 4), (1, i // 4, i % 4)]
    reads = [pltpu.make_async_copy((v_ref, z_ref)[a].at[layer, pl.ds(4 * q, 4)], buf.at[n], rsem.at[n])
             for n, (layer, a, q) in enumerate(order)]
    writes = [pltpu.make_async_copy(buf.at[n], (vo_ref, zo_ref)[a].at[layer, pl.ds(4 * q, 4)], wsem.at[n])
              for n, (layer, a, q) in enumerate(order)]
    part_copies = [pltpu.make_async_copy(part_ref.at[a], part_out.at[a], psem.at[a]) for a in range(2)]
    filt_copies[0].start()
    for n in range(AHEAD):
        reads[n].start()
    filt_copies[1].start()
    done = 0

    def pass_on(upto):
        for n in range(done, upto):
            reads[n].wait()
            writes[n].start()
            if n + AHEAD < 16:
                reads[n + AHEAD].start()

    for i in range(8):
        a, q = divmod(i, 4)
        pass_on(min(2 * i + 3, 16))
        done = min(2 * i + 3, 16)
        if q == 0:
            filt_copies[a].wait()
            shift_filters(fwin.at[a], fsh)
        conv_unit(buf.at[2 * i], fsh, part_ref.at[a, q])
        if q == 3:
            part_copies[a].start()
    for copy in writes + part_copies:
        copy.wait()


def dense_kernel(emb_hbm, state_hbm, b_in_hbm, taps_hbm, skip_hbm, b_out_hbm, part_hbm, v_ref, z_ref, f_ref, w_in_ref, w_out_ref, w_up_ref, w_down_ref,
                 hid_out, state_out, rows_out,
                 emb_ref, state_ref, b_in_ref, taps_ref, skip_ref, b_out_ref,
                 w_in, w_out, w_up, w_down, lags, ext, shifted, xrow, inner, emb,
                 buf, fwin, fsh, part_ref, part_in, rs_out, rs_in, hid, fin, vzp, hid_v, state_v, rows_v,
                 in_sem, lag_sem, out_sem, up_sem, down_sem, own_sem, buf_sem, fwin_sem, fin_sem, small_sem,
                 part_send, part_recv, rs_send, rs_recv, ag_send, ag_recv, fin_send, fin_recv, vzp_send, vzp_recv):
    t = lax.axis_index("tp")
    s = lax.axis_index("sp")
    flip_t = (3 - t, (t + 2) % 4, t + 1 - 2 * (t % 2))
    flip_s = (3 - s, (s + 2) % 4, s + 1 - 2 * (s % 2))
    middle = (t + 1) // 2 % 2
    slot_t = (middle, 1 - middle, 2)
    peer_t = (flip_t[0] + middle * (flip_t[1] - flip_t[0]), flip_t[1] + middle * (flip_t[0] - flip_t[1]), flip_t[2])
    rows = NUM_STEPS * 4
    cols = ext.shape[-1]
    dim = 4 * cols
    width = cols // SUB

    in_copies = [[pltpu.make_async_copy(w_in_ref.at[l, g], w_in.at[l, g], in_sem.at[l, g]) for g in range(3)] for l in range(2)]
    out_copies = [[pltpu.make_async_copy(w_out_ref.at[l, pl.ds(256 * i, 256)], w_out.at[l, pl.ds(256 * i, 256)], out_sem.at[l, i])
                   for i in range(cols // 256)] for l in range(2)]
    up_copies = [[pltpu.make_async_copy(w_up_ref.at[l, pl.ds(512 * i, 512)], w_up.at[l, pl.ds(512 * i, 512)], up_sem.at[l, i])
                  for i in range(4)] for l in range(2)]
    down_copies = [[pltpu.make_async_copy(w_down_ref.at[l, pl.ds(512 * i, 512)], w_down.at[l, pl.ds(512 * i, 512)], down_sem.at[l, i])
                    for i in range(4)] for l in range(2)]
    lag_copy = pltpu.make_async_copy(f_ref.at[:, :, pl.ds(0, 8)], lags, lag_sem)

    def start(copies):
        for copy in copies:
            copy.start()

    def wait(copies):
        for copy in copies:
            copy.wait()

    part_loads = [pltpu.make_async_copy(part_hbm.at[a], part_ref.at[a], own_sem.at[a]) for a in range(2)]
    shard_len = v_ref.shape[2]
    fwin_copies = [pltpu.make_async_copy(f_ref.at[1, a, pl.ds(window_base(shard_len), shard_len + 8)], fwin.at[a], fwin_sem.at[a])
                   for a in range(2)]
    reads = [pltpu.make_async_copy((v_ref, z_ref)[n // 4].at[1, pl.ds(4 * (n % 4), 4)], buf.at[n % 4], buf_sem.at[n]) for n in range(8)]
    small_copies = [pltpu.make_async_copy(src, dst, small_sem.at[i]) for i, (src, dst) in enumerate((
        (emb_hbm, emb_ref), (state_hbm, state_ref), (b_in_hbm, b_in_ref), (taps_hbm, taps_ref), (skip_hbm, skip_ref), (b_out_hbm, b_out_ref)))]
    start(part_loads)
    start(small_copies)
    start(in_copies[0])
    lag_copy.start()

    barrier = pltpu.get_barrier_semaphore()
    for k in range(3):
        pl.semaphore_signal(barrier, inc=1, device_id={"tp": flip_t[k]}, device_id_type=MESH)
        pl.semaphore_signal(barrier, inc=1, device_id={"sp": flip_s[k]}, device_id_type=MESH)
    wait(small_copies)
    for k in range(4):
        @pl.when(s == k)
        def _():
            for j in range(NUM_STEPS):
                for i in range(4):
                    for u in range(SUB):
                        first = cols * i + width * u
                        emb[i, u, 4 * j:4 * j + 4] = emb_ref[j, :, first:first + width].astype(F32)[4 * k:4 * k + 4]
    pl.semaphore_wait(barrier, 6)

    sends = []

    def send(src, dst, send_sem, recv_sem, device_id):
        copy = pltpu.make_async_remote_copy(src_ref=src, dst_ref=dst, send_sem=send_sem, recv_sem=recv_sem,
                                            device_id=device_id, device_id_type=MESH)
        copy.start()
        sends.append(copy)
        return copy

    def send_part(a):
        if a < 2:
            part_loads[a].wait()
        return [send(part_ref.at[a, flip_s[k]], part_in.at[a, k], part_send.at[a, k], part_recv.at[a, k], {"sp": flip_s[k]})
                for k in range(3)]

    part_copies = [send_part(0), send_part(1), None, None]

    def cached_terms(a, first, count):
        if first == 0:
            fwin_copies[a].wait()
            shift_filters(fwin.at[a], fsh)
        for q in range(first, first + count):
            n = 4 * a + q
            reads[n].wait()
            conv_unit(buf.at[q], fsh, part_ref.at[2 + a, q])
            if n + 4 < 8:
                reads[n + 4].start()
        if first + count == 4:
            part_copies[2 + a] = send_part(2 + a)

    def order_rows(l):
        for copy in vzp_copies[l]:
            copy.wait_recv()
        for g in range(4):
            for c in range(3):
                for b in range(4):
                    first = 8 * c + b
                    pair = jnp.concatenate([vzp[g, l, first:first + 1], vzp[g, l, first + 4:first + 5]], axis=0)
                    state_v[l, 4 * g + b, c] = pair.astype(BF16)

        @pl.when(s == 3)
        def _():
            for a in range(2):
                for g in range(4):
                    for b in range(4):
                        first = 24 + 16 * a + b
                        new = [vzp[g, l, first + 4 * j:first + 4 * j + 1] for j in range(NUM_STEPS)]
                        new = jnp.concatenate(new + [jnp.zeros((4, cols), F32)], axis=0)
                        rows_v[a, l, 4 * g + b] = new.astype(BF16)

    def norm_to_xrow(pieces):
        mean = sum(jnp.sum(c, axis=-1, keepdims=True) for c in pieces) / dim
        cent = [c - mean for c in pieces]
        var = sum(jnp.sum(c * c, axis=-1, keepdims=True) for c in cent) / dim
        scale = lax.rsqrt(var + 1e-5)
        for i, c in enumerate(cent):
            xrow[:, width * i:width * (i + 1)] = (c * scale).astype(BF16)

    def reduce_gather(r, act, weight, base_ref, bias_of, out_ref):
        def piece(c, u):
            return jnp.dot(act, weight[:, pl.ds(pl.multiple_of(c * cols + u * width, width), width)], preferred_element_type=F32)

        copies = []
        for u in range(SUB):
            for k, peer in zip(slot_t, peer_t):
                rs_out[r, k, u] = piece(peer, u)
                copies.append(send(rs_out.at[r, k, u], rs_in.at[r, k, u], rs_send.at[r, k, u], rs_recv.at[r, k, u], {"tp": peer}))
        totals = [base_ref[t, u] + piece(t, u) for u in range(SUB)]
        if bias_of is not None:
            totals = [total + bias_of(u) for u, total in enumerate(totals)]
        if r == 0:
            cached_terms(0, 0, 3)
        if r == 1:
            cached_terms(1, 1, 3)
        if r == 2:
            order_rows(0)
        gathers = []
        for u in range(SUB):
            total = totals[u]
            for k in (2, 1, 0):
                copies[3 * u + k].wait_recv()
                total = total + rs_in[r, slot_t[k], u]
            out_ref[t, u] = total
            own = out_ref.at[t, u]
            gathers.append([send(own, own, ag_send.at[r, k, u], ag_recv.at[r, k, u], {"tp": peer}) for k, peer in zip(slot_t, peer_t)])
        if r == 0:
            cached_terms(0, 3, 1)
            cached_terms(1, 0, 1)
        return gathers

    def wait_gather(gathers):
        for copies in gathers:
            for copy in copies:
                copy.wait_recv()

    def pieces_of(ref):
        return [ref[i, u] for i in range(4) for u in range(SUB)]

    vzp_copies = []
    shifted[0:rows, :] = jnp.zeros((rows, cols), F32)
    for l in range(NUM_LAYERS):
        base = emb if l == 0 else hid.at[2 * l - 1]
        norm_to_xrow(pieces_of(base))
        x = xrow[...]
        for g in range(3):
            in_copies[l][g].wait()
            if l == 0 and g == 1:
                start(out_copies[0])
            proj = jnp.dot(x, w_in[l, g], preferred_element_type=F32) + b_in_ref[g, l:l + 1]
            proj = proj.astype(BF16).astype(F32)
            ext[g, 8:24] = proj
            for b in range(4):
                old = state_ref[l, 4 * s + b, g].astype(F32)
                ext[g, b:b + 1] = old[0:1]
                ext[g, 4 + b:5 + b] = old[1:2]
            vzp[s, l, 8 * g:8 * g + 8] = proj[8:16]
        if l == 0:
            start(fwin_copies)
            start(reads[:4])
        start(up_copies[l])
        start(down_copies[l])

        def mixed(g):
            return (taps_ref[0, g, l:l + 1] * ext[g, 8:24] + taps_ref[1, g, l:l + 1] * ext[g, 4:20]
                    + taps_ref[2, g, l:l + 1] * ext[g, 0:16])

        def conv(which, new):
            a = 2 * l + which
            if a == 0:
                lag_copy.wait()
            shifted[rows:2 * rows, :] = new
            acc = skip_ref[l, which:which + 1] * new
            for d in range(NUM_STEPS):
                acc = acc + lags[l, which, d:d + 1] * shifted[rows - 4 * d:2 * rows - 4 * d]
            acc = acc + part_ref[a, s]
            for k in range(3):
                part_copies[a][k].wait_recv()
                acc = acc + part_in[a, k]
            return acc

        v_new = mixed(2).astype(BF16).astype(F32)
        vzp[s, l, 24:40] = v_new
        z_new = (mixed(0) * conv(0, v_new)).astype(BF16).astype(F32)
        vzp[s, l, 40:56] = z_new
        y = (mixed(1) * conv(1, z_new)).astype(BF16)
        wait(out_copies[l])
        bias = [b_out_ref[l:l + 1, pl.ds(pl.multiple_of(t * cols + u * width, width), width)] for u in range(SUB)]
        gathers = reduce_gather(2 * l, y, w_out.at[l], base, lambda u: bias[u], hid.at[2 * l])
        vzp_copies.append([send(vzp.at[s, l], vzp.at[s, l], vzp_send.at[l, k], vzp_recv.at[l, k], {"sp": flip_s[k]}) for k in range(3)])
        if l == 0:
            start(in_copies[1])
            start(out_copies[1])
        wait_gather(gathers)
        norm_to_xrow(pieces_of(hid.at[2 * l]))
        x = xrow[...]
        wait(up_copies[l])
        for i in range(4):
            up = jnp.dot(x, w_up[l, :, cols * i:cols * (i + 1)], preferred_element_type=F32)
            inner[:, cols * i:cols * (i + 1)] = jax.nn.gelu(up).astype(BF16)
        act = inner[...]
        wait(down_copies[l])
        if l == 0:
            wait_gather(reduce_gather(1, act, w_down.at[l], hid.at[0], None, hid.at[1]))
        else:
            gathers = reduce_gather(3, act, w_down.at[l], hid.at[2], None, fin.at[s])

    def place(g, i, u):
        first = pl.multiple_of(cols * i + width * u, width)
        for k in range(4):
            @pl.when(g == k)
            def _():
                for j in range(NUM_STEPS):
                    hid_v[j, 4 * k:4 * k + 4, pl.ds(first, width)] = fin[k, i, u, 4 * j:4 * j + 4]

    chunk_ids = (t,) + peer_t
    order = [(i, u) for u in range(SUB) for i in (0, 3, 2, 1)]
    fin_copies = []
    for i, u in order:
        if i == 3 and u == 0:
            order_rows(1)
            pltpu.make_async_copy(state_v, state_out, fin_sem.at[1]).start()

            @pl.when(s == 3)
            def _():
                pltpu.make_async_copy(rows_v, rows_out, fin_sem.at[2]).start()

        if i > 0:
            gathers[u][i - 1].wait_recv()
        chunk = fin.at[s, chunk_ids[i], u]
        fin_copies.append([send(chunk, chunk, fin_send.at[i, k, u], fin_recv.at[i, k, u], {"sp": flip_s[k]}) for k in (2, 1, 0)])
        place(s, chunk_ids[i], u)
    for n, (i, u) in enumerate(order):
        for k in range(3):
            fin_copies[n][k].wait_recv()
            place(flip_s[2 - k], chunk_ids[i], u)
    hid_copy = pltpu.make_async_copy(hid_v, hid_out, fin_sem.at[0])
    hid_copy.start()
    pltpu.make_async_copy(state_v, state_out, fin_sem.at[1]).wait()

    @pl.when(s == 3)
    def _():
        pltpu.make_async_copy(rows_v, rows_out, fin_sem.at[2]).wait()

    hid_copy.wait()
    for copy in sends:
        copy.wait_send()


def finish_kernel(hid_ref, state_ref, rows_ref, v_ref, z_ref, hid_out, state_out, vo_ref, zo_ref, hid, state, rows, in_sem, out_sem):
    last = lax.axis_index("sp") == 3
    hid_in = [pltpu.make_async_copy(hid_ref.at[j], hid.at[j], in_sem.at[j]) for j in range(NUM_STEPS)]
    hid_put = [pltpu.make_async_copy(hid.at[j], hid_out.at[j], out_sem.at[j]) for j in range(NUM_STEPS)]
    state_in = pltpu.make_async_copy(state_ref, state, in_sem.at[4])
    state_put = pltpu.make_async_copy(state, state_out, out_sem.at[4])
    rows_in = [pltpu.make_async_copy(rows_ref.at[a], rows.at[a], in_sem.at[5 + a]) for a in range(2)]
    rows_put = [pltpu.make_async_copy(rows.at[a], dst.at[:, :, pl.ds(0, 8)], out_sem.at[5 + a]) for a, dst in enumerate((vo_ref, zo_ref))]

    @pl.when(last)
    def _():
        for copy in rows_in:
            copy.start()

    for copy in [state_in] + hid_in:
        copy.start()

    @pl.when(last)
    def _():
        for before, after in zip(rows_in, rows_put):
            before.wait()
            after.start()

    for before, after in zip([state_in] + hid_in, [state_put] + hid_put):
        before.wait()
        after.start()
    for copy in [state_put] + hid_put:
        copy.wait()

    @pl.when(last)
    def _():
        for copy in rows_put:
            copy.wait()


def solution(mesh):
    sp_size = mesh.shape["sp"]

    def device_fn(step_emb, v_cache, z_cache, short_state, w_in, b_in, short_taps, long_filt, skip_gain, w_out, b_out, w_up, w_down):
        num_seq, shard_len, chan = v_cache.shape[1:]
        dim = step_emb.shape[-1]
        own = num_seq // sp_size
        rows = NUM_STEPS * own
        hbm = pl.BlockSpec(memory_space=pl.ANY)
        sds = jax.ShapeDtypeStruct

        v_out, z_out, part = pl.pallas_call(
            conv_kernel,
            name="conv_kernel",
            out_shape=(sds(v_cache.shape, BF16), sds(z_cache.shape, BF16), sds((2, sp_size, rows, chan), F32)),
            in_specs=[hbm] * 3,
            out_specs=(hbm, hbm, hbm),
            scratch_shapes=[
                pltpu.VMEM((16, own, shard_len, chan), BF16),
                pltpu.VMEM((2, shard_len + 8, chan), F32),
                pltpu.VMEM((NUM_STEPS, shard_len, chan), F32),
                pltpu.VMEM((2, sp_size, rows, chan), F32),
                pltpu.SemaphoreType.DMA((16,)),
                pltpu.SemaphoreType.DMA((16,)),
                pltpu.SemaphoreType.DMA((2,)),
                pltpu.SemaphoreType.DMA((2,)),
            ],
            compiler_params=pltpu.CompilerParams(vmem_limit_bytes=VMEM_LIMIT),
        )(v_cache, z_cache, long_filt)

        dma = pltpu.SemaphoreType.DMA
        chunk = (SUB, rows, chan // SUB)
        state_shape = sds((NUM_LAYERS, num_seq, 3, 2, chan), BF16)
        hid_shape = sds((NUM_STEPS, num_seq, dim), F32)
        rows_shape = sds((2, NUM_LAYERS, num_seq, 8, chan), BF16)
        hidden, states, new_rows = pl.pallas_call(
            dense_kernel,
            name="dense_kernel",
            out_shape=(hid_shape, state_shape, rows_shape),
            in_specs=[hbm] * 14,
            out_specs=(hbm, hbm, hbm),
            scratch_shapes=[
                pltpu.VMEM(step_emb.shape, BF16),
                pltpu.VMEM(state_shape.shape, BF16),
                pltpu.VMEM((3, NUM_LAYERS, chan), F32),
                pltpu.VMEM((3, 3, NUM_LAYERS, chan), F32),
                pltpu.VMEM((NUM_LAYERS, 2, chan), F32),
                pltpu.VMEM((NUM_LAYERS, dim), F32),
                pltpu.VMEM((2, 3, dim, chan), BF16),
                pltpu.VMEM((2, chan, dim), BF16),
                pltpu.VMEM((2, dim, w_up.shape[-1]), BF16),
                pltpu.VMEM((2, w_down.shape[1], dim), BF16),
                pltpu.VMEM((2, 2, 8, chan), F32),
                pltpu.VMEM((3, rows + 8, chan), F32),
                pltpu.VMEM((2 * rows, chan), F32),
                pltpu.VMEM((rows, dim), BF16),
                pltpu.VMEM((rows, w_up.shape[-1]), BF16),
                pltpu.VMEM((4,) + chunk, F32),
                pltpu.VMEM((4, own, shard_len, chan), BF16),
                pltpu.VMEM((2, shard_len + 8, chan), F32),
                pltpu.VMEM((NUM_STEPS, shard_len, chan), F32),
                pltpu.VMEM((4, sp_size, rows, chan), F32),
                pltpu.VMEM((4, 3, rows, chan), F32),
                pltpu.VMEM((4, 3) + chunk, F32),
                pltpu.VMEM((4, 3) + chunk, F32),
                pltpu.VMEM((3, 4) + chunk, F32),
                pltpu.VMEM((4, 4) + chunk, F32),
                pltpu.VMEM((4, 2, 56, chan), F32),
                pltpu.VMEM(hid_shape.shape, F32),
                pltpu.VMEM(state_shape.shape, BF16),
                pltpu.VMEM(rows_shape.shape, BF16),
                dma((2, 3)), dma(()), dma((2, 2)), dma((2, 4)), dma((2, 4)), dma((2,)), dma((8,)), dma((2,)), dma((3,)), dma((6,)),
                dma((4, 3)), dma((4, 3)), dma((4, 3, SUB)), dma((4, 3, SUB)), dma((4, 3, SUB)), dma((4, 3, SUB)), dma((4, 3, SUB)), dma((4, 3, SUB)),
                dma((2, 3)), dma((2, 3)),
            ],
            compiler_params=pltpu.CompilerParams(collective_id=0, has_side_effects=True, vmem_limit_bytes=VMEM_LIMIT),
        )(step_emb, jnp.transpose(short_state, (0, 1, 3, 2, 4)), jnp.transpose(b_in, (1, 0, 2)), jnp.transpose(short_taps, (1, 2, 0, 3)),
          skip_gain, b_out, part, v_cache, z_cache, long_filt, jnp.transpose(w_in, (0, 2, 1, 3)), w_out, w_up, w_down)

        hidden, states, v_out, z_out = pl.pallas_call(
            finish_kernel,
            name="finish_kernel",
            out_shape=(hid_shape, state_shape, sds(v_cache.shape, BF16), sds(z_cache.shape, BF16)),
            in_specs=[hbm] * 5,
            out_specs=(hbm,) * 4,
            input_output_aliases={3: 2, 4: 3},
            scratch_shapes=[pltpu.VMEM(hid_shape.shape, F32), pltpu.VMEM(state_shape.shape, BF16), pltpu.VMEM(rows_shape.shape, BF16),
                            dma((7,)), dma((7,))],
            compiler_params=pltpu.CompilerParams(vmem_limit_bytes=VMEM_LIMIT),
        )(hidden, states, new_rows, v_out, z_out)
        return (hidden, v_out, z_out, jnp.transpose(states, (0, 1, 3, 2, 4)))

    specs_in = (
        P(None, "dp", None),
        P(None, "dp", "sp", "tp"),
        P(None, "dp", "sp", "tp"),
        P(None, "dp", None, None, "tp"),
        P(None, None, None, "tp"),
        P(None, None, "tp"),
        P(None, None, None, "tp"),
        P(None, None, None, "tp"),
        P(None, None, "tp"),
        P(None, "tp", None),
        P(None, None),
        P(None, None, "tp"),
        P(None, "tp", None),
    )
    specs_out = (
        P(None, "dp", None),
        P(None, "dp", "sp", "tp"),
        P(None, "dp", "sp", "tp"),
        P(None, "dp", None, None, "tp"),
    )
    return jax.shard_map(device_fn, mesh=mesh, in_specs=specs_in, out_specs=specs_out, check_vma=False)
```
